32 devices in a mesh: tm: 16 (over z, y, x), batch: 2 (over core).
Axes of the slice: x: 2, y: 2, z: 4, core: 2. Of those that a mesh axis runs over, the one named last changes fastest.
Arguments:
- gate_in: bfloat16 [1024, 4096], P('tm', 'batch'), parts along dimension 1, may hold values from -4.5 to 8.75
- cand_in: bfloat16 [1024, 4096], P('tm', 'batch'), parts along dimension 1, may hold values from -6 to 6
- rates: float32 [4096], P('batch'), parts along dimension 0, may hold values from 9.765625e-05 to 0.5
- init_state: float32 [4096], P('batch'), parts along dimension 0, may hold values from -5 to 5
- recur_weight: bfloat16 [2048, 2048], replicated, may hold values from -0.5 to 0.5
Outputs:
- trajectory: float32 [1024, 4096], P('tm', 'batch'), parts along dimension 1
- step_norms: float32 [6], P('batch'), parts along dimension 0
The draws below stay inside these ranges and needn't reach their ends.
There are 2 independent parts, one for each index of `batch`. The reference program is written for one: setup_inputs(seed, part) draws one part's arguments, and reference() takes and returns one part's arrays. A program takes and returns all parts, laid end to end along the dimension named above; an argument that names none is the same for every part. Nothing has to cross between parts.
All inputs are finite; a program needn't handle non-finite values.
Results may differ from the reference program's by a relative error of at most 0.0012.
Values sent between devices are 32-bit elements; how exact they have to be, the bound alone decides.
No kernel may reach another device: no remote copies, remote signals or barrier semaphores. Data moves between devices by JAX's collectives and lax.ppermute only.
A program may use at most 64 MiB of HBM per device.

```python
import jax
import jax.numpy as jnp
from jax import lax

H = 2048
ITERS = 3
TOKENS = 1024


def draw_gate_in(key, part):
    first_key, spot_key, height_key = jax.random.split(jax.random.fold_in(key, 11), 3)
    base = jnp.clip(jax.random.normal(first_key, (TOKENS, H)), -4.0, 4.0)
    spots = jax.random.randint(spot_key, (4,), 0, TOKENS)
    height = jax.random.uniform(height_key, (4,), minval=8.25, maxval=8.7)
    places = jnp.arange(TOKENS)
    level = jnp.max(jnp.where(places[:, None] == spots[None, :], height[None, :], -100.0), axis=1)
    return jnp.where(level[:, None] > 0.0, level[:, None] + 0.0 * base, base).astype(jnp.bfloat16)


def draw_rates(key, part):
    first_key = jax.random.fold_in(jax.random.fold_in(key, 23), 0)
    lowest = jnp.log(0.1 / TOKENS)
    values = jnp.exp(jax.random.uniform(first_key, (H,), minval=lowest, maxval=jnp.log(0.5)))
    return values.astype(jnp.float32)


def draw_recur_weight(key, part):
    body_key, size_key, sign_key = jax.random.split(jax.random.fold_in(key, 37), 3)
    spread = jnp.float32(H) ** (-0.5)
    inner = jnp.clip(jax.random.normal(body_key, (H, H)), -6.0, 6.0) * spread
    size = jnp.exp(jax.random.uniform(size_key, (H,), minval=jnp.log(0.2), maxval=jnp.log(0.5)))
    sign = jnp.where(jax.random.uniform(sign_key, (H,)) < 0.5, -1.0, 1.0)
    places = jnp.arange(H)
    on_diag = places[:, None] == places[None, :]
    values = jnp.where(on_diag, (size * sign)[:, None] + 0.0 * inner, inner)
    return values.astype(jnp.float32).astype(jnp.bfloat16)


def steps_of(own_key, extent, shards, low, largest):
    def one(position, blocks):
        steps = jax.random.uniform(jax.random.fold_in(jax.random.fold_in(own_key, 6), position), (blocks,), jnp.float32, low / len(shards), largest / len(shards))
        return jnp.repeat(jnp.exp(steps), extent[position] // blocks).reshape((-1,) + (1,) * (len(extent) - position - 1))

    gain = one(*shards[0])
    for cut in shards[1:]:
        gain = gain * one(*cut)
    return gain


def normal_values(rng, dims, scale, limit, shards=(), dtype=jnp.bfloat16):
    drawn = jax.random.normal(rng, dims, jnp.float32) * scale
    if len(shards) > 0:
        drawn = steps_of(rng, dims, shards, -0.22, 0.18) * drawn
    return jnp.clip(drawn, min=-limit, max=limit).astype(dtype)


def setup_inputs(seed: int = 0, part: int = 0) -> dict:
    seeds = jax.random.split(jax.random.key(seed), 6)
    part_keys = jax.random.split(jax.random.fold_in(seeds[5], part), 6)
    return {
        "gate_in": draw_gate_in(jax.random.fold_in(jax.random.fold_in(seeds[5], part), 71), part),
        "cand_in": normal_values(part_keys[1], (TOKENS, H), 1.0, 6.0, ((0, 16),)),
        "rates": draw_rates(jax.random.fold_in(jax.random.fold_in(seeds[5], part), 71), part),
        "init_state": normal_values(part_keys[3], (H,), 1.0, 5.0, (), jnp.float32),
        "recur_weight": draw_recur_weight(jax.random.fold_in(seeds[5], 71), part),
    }


def link(earlier, later):
    return (later[0] * earlier[0], later[0] * earlier[1] + later[1])

def reference(gate_in, cand_in, rates, init_state, recur_weight):
    gate = gate_in.astype(jnp.float32)
    keep = jnp.exp(-rates[None, :] * jax.nn.softplus(gate) - jnp.maximum(gate - 8.0, 0.0))
    cand_base = cand_in.astype(jnp.float32)
    unit_diag = jnp.diagonal(recur_weight).astype(jnp.float32)
    state = jnp.zeros(gate.shape, jnp.float32)
    totals = []
    for step in range(ITERS):
        prev = jnp.concatenate([init_state[None, :], state[:-1]], axis=0)
        mixed = jnp.dot(prev.astype(jnp.bfloat16), recur_weight, preferred_element_type=jnp.float32)
        cand = jnp.tanh(cand_base + mixed)
        mapped = keep * prev + (1.0 - keep) * cand
        slope = keep + (1.0 - keep) * (1.0 - cand * cand) * unit_diag[None, :]
        offset = mapped - slope * prev
        offset = jnp.concatenate([offset[:1] + slope[:1] * init_state[None, :], offset[1:]], axis=0)
        cum_a, fresh = lax.associative_scan(link, (slope, offset), axis=0)
        delta = fresh - state
        totals.append(jnp.sum(delta * delta))
        state = fresh
    return (state, jnp.sqrt(jnp.stack(totals) / (TOKENS * H)))
```

```python
import functools

import jax
import jax.numpy as jnp
from jax import lax
from jax.experimental import pallas as pl
from jax.experimental.pallas import tpu as pltpu
from jax.sharding import PartitionSpec as P

SUB = 8
LANE = 128
WIDE = 256
VMEM_LIMIT = 16 * 1024 * 1024
F32 = jnp.float32
BF16 = jnp.bfloat16


def softplus(x):
    return jnp.maximum(x, 0.0) + jnp.log1p(jnp.exp(-jnp.abs(x)))


def chunk_scan(mul, add):
    run_a, run_b = [mul[0]], [add[0]]
    for a, b in zip(mul[1:], add[1:]):
        run_a.append(a * run_a[-1])
        run_b.append(a * run_b[-1] + b)
    tot_a, tot_b = run_a[-1], run_b[-1]
    place = lax.broadcasted_iota(jnp.int32, tot_a.shape, 0)
    shift = 1
    while shift < SUB:
        far = place >= shift
        old_a = jnp.where(far, pltpu.roll(tot_a, shift, 0), 1.0)
        old_b = jnp.where(far, pltpu.roll(tot_b, shift, 0), 0.0)
        tot_b = tot_a * old_b + tot_b
        tot_a = tot_a * old_a
        shift *= 2
    far = place >= 1
    head_a = jnp.where(far, pltpu.roll(tot_a, 1, 0), 1.0)
    head_b = jnp.where(far, pltpu.roll(tot_b, 1, 0), 0.0)
    cum_a = [a * head_a for a in run_a]
    cum_b = [a * head_b + b for a, b in zip(run_a, run_b)]
    return cum_a, cum_b


def write_rows(ref, base, first_tile, row):
    for k in range(row.shape[1] // LANE):
        ref[pl.ds(base + first_tile + k, 1), :] = row[:, k * LANE : (k + 1) * LANE]


def read_row(ref, first_tile, tiles):
    return jnp.concatenate([ref[pl.ds(first_tile + k, 1), :] for k in range(tiles)], axis=1)


def spread(one_ref, out_ref):
    value = one_ref[...]
    for q in range(out_ref.shape[0]):
        out_ref[q] = value


def start_kernel(
    me_ref, gate_ref, cand_ref, rates_ref, init_ref, w_hbm,
    w_ref, keep_ref, base_ref, cum_a_ref, cum_b_ref, diag_ref, pay_ref,
    blocks, keep_nat, base_nat, mul_nat, add_nat, one, w_sem, d_sem,
):
    rows, width = gate_ref.shape
    steps = rows // SUB
    tiles = width // LANE
    parts = 8
    part = width // parts
    diag_copies = [
        pltpu.make_async_copy(
            w_hbm.at[pl.ds(k * LANE, LANE), pl.ds(k * LANE, LANE)], blocks.at[k], d_sem.at[k]
        )
        for k in range(tiles)
    ]
    w_copies = [
        pltpu.make_async_copy(
            w_hbm.at[pl.ds(k * part, part), :], w_ref.at[pl.ds(k * part, part), :], w_sem.at[k]
        )
        for k in range(parts)
    ]
    for copy in diag_copies:
        copy.start()
    for copy in w_copies:
        copy.start()

    per = WIDE // LANE

    def split(ref, j, value):
        for k in range(per):
            ref[j * per + k] = value[:, k * LANE : (k + 1) * LANE]

    def joined(ref, j, at):
        return jnp.concatenate([ref[j * per + k, at, :] for k in range(per)], axis=1)

    @pl.loop(0, width // WIDE)
    def _(j):
        cols = pl.ds(pl.multiple_of(j * WIDE, WIDE), WIDE)
        gate = gate_ref[:, cols].astype(F32)
        split(keep_nat, j, jnp.exp(-rates_ref[:, cols] * softplus(gate) - jnp.maximum(gate - 8.0, 0.0)))

    for copy in diag_copies:
        copy.wait()
    on_diag = lax.broadcasted_iota(jnp.int32, (LANE, LANE), 0) == lax.broadcasted_iota(jnp.int32, (LANE, LANE), 1)
    for k in range(tiles):
        block = blocks[k].astype(F32)
        diag_ref[:, k * LANE : (k + 1) * LANE] = jnp.sum(jnp.where(on_diag, block, 0.0), axis=0, keepdims=True)

    @pl.loop(0, width // WIDE)
    def _(j):
        cols = pl.ds(pl.multiple_of(j * WIDE, WIDE), WIDE)
        keep = joined(keep_nat, j, slice(None))
        base = cand_ref[:, cols].astype(F32)
        cand = jnp.tanh(base)
        left = 1.0 - keep
        split(mul_nat, j, keep + left * (1.0 - cand * cand) * diag_ref[:, cols])
        split(add_nat, j, left * cand)
        split(base_nat, j, base)

    @pl.when(me_ref[0] == 0)
    def _():
        total = jnp.zeros((SUB, width), F32)
        for k in range(parts):
            w_copies[k].wait()
            left = jnp.broadcast_to(init_ref[:, k * part : (k + 1) * part], (SUB, part)).astype(BF16)
            total = total + jnp.dot(left, w_ref[k * part : (k + 1) * part, :], preferred_element_type=F32)
        for j in range(tiles):
            here = slice(j * LANE, (j + 1) * LANE)
            prev = init_ref[:, here]
            keep = keep_nat[j, 0:1, :]
            cand = jnp.tanh(base_nat[j, 0:1, :] + total[0:1, here])
            mapped = keep * prev + (1.0 - keep) * cand
            slope = keep + (1.0 - keep) * (1.0 - cand * cand) * diag_ref[:, here]
            mul_nat[j, 0:1, :] = slope
            add_nat[j, 0:1, :] = mapped - slope * prev

    @pl.when(me_ref[0] != 0)
    def _():
        for copy in w_copies:
            copy.wait()

    @pl.loop(0, width // WIDE)
    def _(j):
        cols = pl.ds(pl.multiple_of(j * WIDE, WIDE), WIDE)
        turn = [pl.ds(r, SUB, stride=steps) for r in range(steps)]
        cum_a, cum_b = chunk_scan([joined(mul_nat, j, at) for at in turn], [joined(add_nat, j, at) for at in turn])
        for r in range(steps):
            here = pl.ds(r * SUB, SUB)
            cum_a_ref[here, cols] = cum_a[r]
            cum_b_ref[here, cols] = cum_b[r]
            keep_ref[here, cols] = joined(keep_nat, j, turn[r])
            base_ref[here, cols] = joined(base_nat, j, turn[r])
        write_rows(one, 0, j * per, cum_a[-1][SUB - 1 :, :])
        write_rows(one, tiles, j * per, cum_b[-1][SUB - 1 :, :])

    spread(one, pay_ref)


def step_kernel(
    last, me_ref, got_ref, init_ref, keep_ref, base_ref, cum_a_ref, cum_b_ref, diag_ref, w_ref, old_ref, tot_ref,
    *rest,
):
    if last:
        fresh_ref, out_a_ref, pay_ref, prev, low, entry, one, acc = rest
    else:
        state_ref, out_a_ref, out_b_ref, sum_ref, pay_ref, prev, low, entry, one, acc = rest
    rows, width = keep_ref.shape
    steps = rows // SUB
    tiles = width // LANE
    per = WIDE // LANE

    def pull(q, e):
        return got_ref[q, 0:tiles, :] * e + got_ref[q, tiles : 2 * tiles, :]

    entry[...] = lax.fori_loop(0, me_ref[0], pull, init_ref[...])
    acc[...] = jnp.zeros_like(acc)

    def turned_state(j, _):
        cols = pl.ds(pl.multiple_of(j * WIDE, WIDE), WIDE)
        e = read_row(entry, j * per, per)
        state = [
            cum_b_ref[pl.ds(r * SUB, SUB), cols] + cum_a_ref[pl.ds(r * SUB, SUB), cols] * e for r in range(steps)
        ]
        place = lax.broadcasted_iota(jnp.int32, state[0].shape, 0)
        before = [jnp.where(place == 0, jnp.broadcast_to(e, state[0].shape), pltpu.roll(state[-1], 1, 0))] + state[:-1]
        moved = 0.0
        for r in range(steps):
            prev[pl.ds(r * SUB, SUB), cols] = before[r]
            change = state[r] if old_ref is None else state[r] - old_ref[pl.ds(r * SUB, SUB), cols]
            moved = moved + change * change
            if not last:
                state_ref[pl.ds(r * SUB, SUB), cols] = state[r]
        for r in range(0, steps, 2):
            low[pl.ds(r * SUB, 2 * SUB), cols] = jnp.concatenate(before[r : r + 2], axis=0).astype(BF16)
        acc[...] += sum(moved[:, k * LANE : (k + 1) * LANE] for k in range(per))
        return 0

    lax.fori_loop(0, width // WIDE, turned_state, 0)
    if not last:
        sum_ref[...] = acc[...]
    else:
        one[pl.ds(4 * tiles, SUB), :] = jnp.zeros((SUB, LANE), F32)
        one[pl.ds(4 * tiles, 1), :] = jnp.sum(tot_ref[...], axis=0, keepdims=True)
        one[pl.ds(4 * tiles + 1, 1), :] = jnp.sum(acc[...], axis=0, keepdims=True)
        acc[...] = jnp.zeros_like(acc)

    def solve(j, _):
        cols = pl.ds(pl.multiple_of(j * WIDE, WIDE), WIDE)
        mixed = jnp.dot(low[...], w_ref[:, cols], preferred_element_type=F32)
        unit = diag_ref[:, cols]
        mul, add = [], []
        for r in range(steps):
            here = pl.ds(r * SUB, SUB)
            keep = keep_ref[here, cols]
            before = prev[here, cols]
            cand = jnp.tanh(base_ref[here, cols] + mixed[r * SUB : (r + 1) * SUB, :])
            left = 1.0 - keep
            mapped = keep * before + left * cand
            slope = keep + left * (1.0 - cand * cand) * unit
            mul.append(slope)
            add.append(mapped - slope * before)
        cum_a, cum_b = chunk_scan(mul, add)
        if last:
            e = read_row(entry, j * per, per)
            c0, c1, c2 = 0.0, 0.0, 0.0
            for r in range(steps):
                here = pl.ds(r * SUB, SUB)
                fresh = cum_b[r] + cum_a[r] * e
                if r + 1 < steps:
                    state = prev[pl.ds((r + 1) * SUB, SUB), cols]
                else:
                    state = cum_b_ref[here, cols] + cum_a_ref[here, cols] * e
                u = fresh - state
                fresh_ref[here, cols] = fresh
                out_a_ref[here, cols] = cum_a[r]
                c0 = c0 + u * u
                c1 = c1 + u * cum_a[r]
                c2 = c2 + cum_a[r] * cum_a[r]
            acc[...] += sum(c0[:, k * LANE : (k + 1) * LANE] for k in range(per))
            write_rows(one, 0, j * per, cum_a[-1][SUB - 1 :, :])
            write_rows(one, tiles, j * per, u[SUB - 1 :, :])
            write_rows(one, 2 * tiles, j * per, 2.0 * jnp.sum(c1, axis=0, keepdims=True))
            write_rows(one, 3 * tiles, j * per, jnp.sum(c2, axis=0, keepdims=True))
        else:
            for r in range(steps):
                here = pl.ds(r * SUB, SUB)
                out_a_ref[here, cols] = cum_a[r]
                out_b_ref[here, cols] = cum_b[r]
            write_rows(one, 0, j * per, cum_a[-1][SUB - 1 :, :])
            write_rows(one, tiles, j * per, cum_b[-1][SUB - 1 :, :])
        return 0

    lax.fori_loop(0, width // WIDE, solve, 0)
    if last:
        one[pl.ds(4 * tiles + 2, 1), :] = jnp.sum(acc[...], axis=0, keepdims=True)
    spread(one, pay_ref)


def first_step_kernel(me, got, init, keep, base, cum_a, cum_b, diag, w, *rest):
    step_kernel(False, me, got, init, keep, base, cum_a, cum_b, diag, w, None, None, *rest)


def final_kernel(me_ref, got_ref, fresh_ref, cum_a_ref, path_ref, norm_ref, entry, nat, quad_ref):
    rows, width = fresh_ref.shape
    steps = rows // SUB
    tiles = width // LANE
    peers = got_ref.shape[0]
    quad_ref[...] = jnp.zeros_like(quad_ref)
    entry[...] = jnp.zeros_like(entry)

    def pull(q, carry):
        d, quad, sums = carry

        @pl.when(q == me_ref[0])
        def _():
            entry[...] = d

        a, b = got_ref[q, 0:tiles, :], got_ref[q, tiles : 2 * tiles, :]
        c1, c2 = got_ref[q, 2 * tiles : 3 * tiles, :], got_ref[q, 3 * tiles : 4 * tiles, :]
        quad = quad + d * (c1 + c2 * d)
        sums = sums + got_ref[q, 4 * tiles : 4 * tiles + SUB, :]
        return a * d + b, quad, sums

    _, quad, sums = lax.fori_loop(0, peers, pull, (entry[...], quad_ref[0:tiles, :], quad_ref[tiles:, :]))
    count = peers * rows * width
    extra = jnp.sum(quad, axis=0, keepdims=True)
    totals = [sums[0:1, :], sums[1:2, :], sums[2:3, :] + extra]
    for k, row in enumerate(totals):
        total = jnp.sum(row, axis=1, keepdims=True)
        norm_ref[k] = jnp.max(jnp.sqrt(total / count))

    @pl.loop(0, tiles)
    def _(j):
        cols = pl.ds(pl.multiple_of(j * LANE, LANE), LANE)
        e = entry[pl.ds(j, 1), :]
        for r in range(steps):
            here = pl.ds(r * SUB, SUB)
            nat[j, pl.ds(r, SUB, stride=steps), :] = fresh_ref[here, cols] + cum_a_ref[here, cols] * e
        path_ref[:, cols] = nat[j]


def exchange(pay):
    return lax.all_to_all(pay, "tm", 0, 0)


def body(gate_in, cand_in, rates, init_state, recur_weight):
    rows, width = gate_in.shape
    peers = lax.axis_size("tm")
    tiles = width // LANE
    steps = rows // SUB
    assert rows % (2 * SUB) == 0 and width % WIDE == 0
    me = lax.axis_index("tm").astype(jnp.int32).reshape(1)
    init_row = init_state.reshape(1, width)
    init_tile = init_state.reshape(tiles, LANE)
    vmem = pl.BlockSpec(memory_space=pltpu.VMEM)
    smem = pl.BlockSpec(memory_space=pltpu.SMEM)
    hbm = pl.BlockSpec(memory_space=pl.ANY)
    grid_f32 = jax.ShapeDtypeStruct((rows, width), F32)
    pay2 = jax.ShapeDtypeStruct((peers, 2 * tiles, LANE), F32)
    pay4 = jax.ShapeDtypeStruct((peers, 4 * tiles + SUB, LANE), F32)

    w, keep, base, cum_a, cum_b, diag, pay = pl.pallas_call(
        start_kernel,
        out_shape=(
            pltpu.VMEM((width, width), BF16),
            grid_f32, grid_f32, grid_f32, grid_f32,
            jax.ShapeDtypeStruct((1, width), F32),
            pay2,
        ),
        in_specs=[smem, vmem, vmem, vmem, vmem, hbm],
        out_specs=(vmem,) * 7,
        scratch_shapes=[
            pltpu.VMEM((tiles, LANE, LANE), BF16),
            pltpu.VMEM((tiles, rows, LANE), F32),
            pltpu.VMEM((tiles, rows, LANE), F32),
            pltpu.VMEM((tiles, rows, LANE), F32),
            pltpu.VMEM((tiles, rows, LANE), F32),
            pltpu.VMEM((2 * tiles, LANE), F32),
            pltpu.SemaphoreType.DMA((8,)),
            pltpu.SemaphoreType.DMA((tiles,)),
        ],
        compiler_params=pltpu.CompilerParams(vmem_limit_bytes=VMEM_LIMIT),
        name="start",
    )(me, gate_in, cand_in, rates.reshape(1, width), init_row, recur_weight)
    got = exchange(pay)

    scratch = [
        pltpu.VMEM((rows, width), F32),
        pltpu.VMEM((rows, width), BF16),
        pltpu.VMEM((tiles, LANE), F32),
    ]
    state, cum_a, cum_b, moved, pay = pl.pallas_call(
        first_step_kernel,
        out_shape=(grid_f32, grid_f32, grid_f32, jax.ShapeDtypeStruct((SUB, LANE), F32), pay2),
        in_specs=[smem] + [vmem] * 8,
        out_specs=(vmem,) * 5,
        scratch_shapes=scratch + [pltpu.VMEM((2 * tiles, LANE), F32), pltpu.VMEM((SUB, LANE), F32)],
        compiler_params=pltpu.CompilerParams(vmem_limit_bytes=VMEM_LIMIT),
        name="middle",
    )(me, got, init_tile, keep, base, cum_a, cum_b, diag, w)
    got = exchange(pay)

    fresh, cum_a, pay = pl.pallas_call(
        functools.partial(step_kernel, True),
        out_shape=(grid_f32, grid_f32, pay4),
        in_specs=[smem] + [vmem] * 10,
        out_specs=(vmem,) * 3,
        scratch_shapes=scratch + [pltpu.VMEM((4 * tiles + SUB, LANE), F32), pltpu.VMEM((SUB, LANE), F32)],
        compiler_params=pltpu.CompilerParams(vmem_limit_bytes=VMEM_LIMIT),
        name="last",
    )(me, got, init_tile, keep, base, cum_a, cum_b, diag, w, state, moved)
    got = exchange(pay)

    path, norms = pl.pallas_call(
        final_kernel,
        out_shape=(grid_f32, jax.ShapeDtypeStruct((3,), F32)),
        in_specs=[smem] + [vmem] * 3,
        out_specs=(vmem, smem),
        scratch_shapes=[
            pltpu.VMEM((tiles, LANE), F32),
            pltpu.VMEM((tiles, rows, LANE), F32),
            pltpu.VMEM((tiles + SUB, LANE), F32),
        ],
        compiler_params=pltpu.CompilerParams(vmem_limit_bytes=VMEM_LIMIT),
        name="final",
    )(me, got, fresh, cum_a)
    return path, norms


def solution(mesh):
    placed = (P("tm", "batch"), P("tm", "batch"), P("batch"), P("batch"), P())
    return jax.shard_map(
        body, mesh=mesh, in_specs=placed, out_specs=(P("tm", "batch"), P("batch")), check_vma=False
    )
```

```python
import functools

import jax
import jax.numpy as jnp
from jax import lax
from jax.experimental import pallas as pl
from jax.experimental.pallas import tpu as pltpu
from jax.sharding import PartitionSpec as P

SUB = 8
LANE = 128
WIDE = 256
PARTS = 4
VMEM_LIMIT = 16 * 1024 * 1024
F32 = jnp.float32
BF16 = jnp.bfloat16


def softplus(x):
    return jnp.maximum(x, 0.0) + jnp.log1p(jnp.exp(-jnp.abs(x)))


def chunk_scan(mul, add):
    run_a, run_b = [mul[0]], [add[0]]
    for a, b in zip(mul[1:], add[1:]):
        run_a.append(a * run_a[-1])
        run_b.append(a * run_b[-1] + b)
    tot_a, tot_b = run_a[-1], run_b[-1]
    place = lax.broadcasted_iota(jnp.int32, tot_a.shape, 0)
    shift = 1
    while shift < SUB:
        far = place >= shift
        old_a = jnp.where(far, pltpu.roll(tot_a, shift, 0), 1.0)
        old_b = jnp.where(far, pltpu.roll(tot_b, shift, 0), 0.0)
        tot_b = tot_a * old_b + tot_b
        tot_a = tot_a * old_a
        shift *= 2
    far = place >= 1
    head_a = jnp.where(far, pltpu.roll(tot_a, 1, 0), 1.0)
    head_b = jnp.where(far, pltpu.roll(tot_b, 1, 0), 0.0)
    cum_a = [a * head_a for a in run_a]
    cum_b = [a * head_b + b for a, b in zip(run_a, run_b)]
    return cum_a, cum_b


def write_rows(ref, base, first_tile, row):
    for k in range(row.shape[1] // LANE):
        ref[pl.ds(base + first_tile + k, 1), :] = row[:, k * LANE : (k + 1) * LANE]


def read_row(ref, first_tile, tiles):
    return jnp.concatenate([ref[pl.ds(first_tile + k, 1), :] for k in range(tiles)], axis=1)


def spread(one_ref, out_ref):
    value = one_ref[...]
    for q in range(out_ref.shape[0]):
        out_ref[q] = value


def start_kernel(
    me_ref, gate_hbm, cand_hbm, rates_hbm, init_hbm, w_hbm,
    keep_ref, base_ref, cum_a_ref, cum_b_ref, diag_ref, pay_ref,
    gate_ref, cand_ref, rates_ref, init_ref, w_ref, blocks, gate_nat, base_nat, mixed, one,
    in_sem, w_sem, d_sem,
):
    rows, width = gate_ref.shape
    steps = rows // SUB
    tiles = width // LANE
    per = WIDE // LANE
    part = width // PARTS
    me = me_ref[0]

    def columns(hbm, ref, k, sem):
        cols = pl.ds(k * part, part)
        return pltpu.make_async_copy(hbm.at[:, cols], ref.at[:, cols], sem)

    rates_copy = pltpu.make_async_copy(rates_hbm, rates_ref, in_sem.at[2 * PARTS])
    init_copy = pltpu.make_async_copy(init_hbm, init_ref, in_sem.at[2 * PARTS + 1])
    gate_copies = [columns(gate_hbm, gate_ref, k, in_sem.at[k]) for k in range(PARTS)]
    cand_copies = [columns(cand_hbm, cand_ref, k, in_sem.at[PARTS + k]) for k in range(PARTS)]
    diag_copies = [
        pltpu.make_async_copy(
            w_hbm.at[pl.ds(k * LANE, LANE), pl.ds(k * LANE, LANE)], blocks.at[k], d_sem.at[k]
        )
        for k in range(tiles)
    ]
    w_copies = [
        pltpu.make_async_copy(
            w_hbm.at[pl.ds(k * part, part), :], w_ref.at[pl.ds(k * part, part), :], w_sem.at[k]
        )
        for k in range(PARTS)
    ]
    rates_copy.start()
    for k in range(PARTS):
        gate_copies[k].start()
        cand_copies[k].start()
    init_copy.start()
    for copy in diag_copies:
        copy.start()

    @pl.when(me == 0)
    def _():
        for copy in w_copies:
            copy.start()

    mixed[...] = jnp.zeros_like(mixed)
    rates_copy.wait()
    turn = [pl.ds(r, SUB, stride=steps) for r in range(steps)]
    for k in range(PARTS):
        gate_copies[k].wait()
        cand_copies[k].wait()

        @pl.loop(k * (part // LANE), (k + 1) * (part // LANE))
        def _(j):
            cols = pl.ds(pl.multiple_of(j * LANE, LANE), LANE)
            gate_nat[j] = gate_ref[:, cols].astype(F32)
            base_nat[j] = cand_ref[:, cols].astype(F32)
            rate = rates_ref[:, cols]
            for r in range(steps):
                here = pl.ds(r * SUB, SUB)
                gate = gate_nat[j, turn[r], :]
                keep_ref[here, cols] = jnp.exp(-rate * softplus(gate) - jnp.maximum(gate - 8.0, 0.0))
                base_ref[here, cols] = base_nat[j, turn[r], :]

    for copy in diag_copies:
        copy.wait()
    on_diag = lax.broadcasted_iota(jnp.int32, (LANE, LANE), 0) == lax.broadcasted_iota(jnp.int32, (LANE, LANE), 1)
    for k in range(tiles):
        block = blocks[k].astype(F32)
        diag_ref[:, k * LANE : (k + 1) * LANE] = jnp.sum(jnp.where(on_diag, block, 0.0), axis=0, keepdims=True)
    init_copy.wait()

    @pl.when(me == 0)
    def _():
        total = jnp.zeros((SUB, width), F32)
        for k in range(PARTS):
            w_copies[k].wait()
            left = jnp.broadcast_to(init_ref[:, k * part : (k + 1) * part], (SUB, part)).astype(BF16)
            total = total + jnp.dot(left, w_ref[k * part : (k + 1) * part, :], preferred_element_type=F32)
        mixed[...] = total[0:1, :]

    @pl.when(me != 0)
    def _():
        init_ref[...] = jnp.zeros_like(init_ref)

    @pl.loop(0, width // WIDE)
    def _(j):
        cols = pl.ds(pl.multiple_of(j * WIDE, WIDE), WIDE)
        top = lax.broadcasted_iota(jnp.int32, (SUB, WIDE), 0) == 0
        unit = diag_ref[:, cols]
        mul, add = [], []
        for r in range(steps):
            here = pl.ds(r * SUB, SUB)
            keep = keep_ref[here, cols]
            left = 1.0 - keep
            base = base_ref[here, cols]
            cand = jnp.tanh(base + jnp.where(top, mixed[:, cols], 0.0) if r == 0 else base)
            slope = keep + left * (1.0 - cand * cand) * unit
            offset = left * cand
            if r == 0:
                prev = jnp.where(top, init_ref[:, cols], 0.0)
                offset = (keep * prev + offset) - slope * prev
            mul.append(slope)
            add.append(offset)
        cum_a, cum_b = chunk_scan(mul, add)
        for r in range(steps):
            here = pl.ds(r * SUB, SUB)
            cum_a_ref[here, cols] = cum_a[r]
            cum_b_ref[here, cols] = cum_b[r]
        write_rows(one, 0, j * per, cum_a[-1][SUB - 1 :, :])
        write_rows(one, tiles, j * per, cum_b[-1][SUB - 1 :, :])

    spread(one, pay_ref)


def step_kernel(
    last, me_ref, got_ref, init_ref, keep_ref, base_ref, cum_a_ref, cum_b_ref, diag_ref, w_ref, old_ref, tot_ref,
    *rest,
):
    if last:
        fresh_ref, out_a_ref, pay_ref, sums_ref, prev, low, entry, one, acc, more = rest
    else:
        state_ref, out_a_ref, out_b_ref, sum_ref, pay_ref, prev, low, entry, one, acc = rest
    rows, width = keep_ref.shape
    steps = rows // SUB
    tiles = width // LANE
    per = WIDE // LANE

    def pull(q, e):
        return got_ref[q, 0:tiles, :] * e + got_ref[q, tiles : 2 * tiles, :]

    entry[...] = lax.fori_loop(0, me_ref[0], pull, init_ref[...])
    acc[...] = jnp.zeros_like(acc)

    def turned_state(j, _):
        cols = pl.ds(pl.multiple_of(j * WIDE, WIDE), WIDE)
        e = read_row(entry, j * per, per)
        state = [
            cum_b_ref[pl.ds(r * SUB, SUB), cols] + cum_a_ref[pl.ds(r * SUB, SUB), cols] * e for r in range(steps)
        ]
        place = lax.broadcasted_iota(jnp.int32, state[0].shape, 0)
        before = [jnp.where(place == 0, jnp.broadcast_to(e, state[0].shape), pltpu.roll(state[-1], 1, 0))] + state[:-1]
        moved = 0.0
        for r in range(steps):
            prev[pl.ds(r * SUB, SUB), cols] = before[r]
            change = state[r] if old_ref is None else state[r] - old_ref[pl.ds(r * SUB, SUB), cols]
            moved = moved + change * change
            if not last:
                state_ref[pl.ds(r * SUB, SUB), cols] = state[r]
        for r in range(0, steps, 2):
            low[pl.ds(r * SUB, 2 * SUB), cols] = jnp.concatenate(before[r : r + 2], axis=0).astype(BF16)
        acc[...] += sum(moved[:, k * LANE : (k + 1) * LANE] for k in range(per))
        return 0

    lax.fori_loop(0, width // WIDE, turned_state, 0)
    if not last:
        sum_ref[...] = acc[...]
    else:
        more[pl.ds(2 * tiles, SUB), :] = jnp.zeros((SUB, LANE), F32)
        more[pl.ds(2 * tiles, 1), :] = jnp.sum(tot_ref[...], axis=0, keepdims=True)
        more[pl.ds(2 * tiles + 1, 1), :] = jnp.sum(acc[...], axis=0, keepdims=True)
        acc[...] = jnp.zeros_like(acc)

    def solve(j, _):
        cols = pl.ds(pl.multiple_of(j * WIDE, WIDE), WIDE)
        mixed = jnp.dot(low[...], w_ref[:, cols], preferred_element_type=F32)
        unit = diag_ref[:, cols]
        mul, add = [], []
        for r in range(steps):
            here = pl.ds(r * SUB, SUB)
            keep = keep_ref[here, cols]
            before = prev[here, cols]
            cand = jnp.tanh(base_ref[here, cols] + mixed[r * SUB : (r + 1) * SUB, :])
            left = 1.0 - keep
            mapped = keep * before + left * cand
            slope = keep + left * (1.0 - cand * cand) * unit
            mul.append(slope)
            add.append(mapped - slope * before)
        cum_a, cum_b = chunk_scan(mul, add)
        if last:
            e = read_row(entry, j * per, per)
            c0, c1, c2 = 0.0, 0.0, 0.0
            for r in range(steps):
                here = pl.ds(r * SUB, SUB)
                fresh = cum_b[r] + cum_a[r] * e
                if r + 1 < steps:
                    state = prev[pl.ds((r + 1) * SUB, SUB), cols]
                else:
                    state = cum_b_ref[here, cols] + cum_a_ref[here, cols] * e
                u = fresh - state
                fresh_ref[here, cols] = fresh
                out_a_ref[here, cols] = cum_a[r]
                c0 = c0 + u * u
                c1 = c1 + u * cum_a[r]
                c2 = c2 + cum_a[r] * cum_a[r]
            acc[...] += sum(c0[:, k * LANE : (k + 1) * LANE] for k in range(per))
            write_rows(one, 0, j * per, cum_a[-1][SUB - 1 :, :])
            write_rows(one, tiles, j * per, u[SUB - 1 :, :])
            write_rows(more, 0, j * per, 2.0 * jnp.sum(c1, axis=0, keepdims=True))
            write_rows(more, tiles, j * per, jnp.sum(c2, axis=0, keepdims=True))
        else:
            for r in range(steps):
                here = pl.ds(r * SUB, SUB)
                out_a_ref[here, cols] = cum_a[r]
                out_b_ref[here, cols] = cum_b[r]
            write_rows(one, 0, j * per, cum_a[-1][SUB - 1 :, :])
            write_rows(one, tiles, j * per, cum_b[-1][SUB - 1 :, :])
        return 0

    lax.fori_loop(0, width // WIDE, solve, 0)
    if last:
        more[pl.ds(2 * tiles + 2, 1), :] = jnp.sum(acc[...], axis=0, keepdims=True)
        spread(more, sums_ref)
    spread(one, pay_ref)


def first_step_kernel(me, got, init, keep, base, cum_a, cum_b, diag, w, *rest):
    step_kernel(False, me, got, init, keep, base, cum_a, cum_b, diag, w, None, None, *rest)


def path_kernel(me_ref, got_ref, fresh_ref, cum_a_ref, path_ref, moves_ref, nat):
    rows, width = fresh_ref.shape
    steps = rows // SUB
    tiles = width // LANE
    peers = got_ref.shape[0]
    moves_ref[0] = jnp.zeros((tiles, LANE), F32)

    def pull(q, d):
        d = got_ref[q, 0:tiles, :] * d + got_ref[q, tiles : 2 * tiles, :]
        moves_ref[q + 1] = d
        return d

    lax.fori_loop(0, peers - 1, pull, moves_ref[0])

    @pl.loop(0, tiles)
    def _(j):
        cols = pl.ds(pl.multiple_of(j * LANE, LANE), LANE)
        e = moves_ref[me_ref[0], pl.ds(j, 1), :]
        for r in range(steps):
            here = pl.ds(r * SUB, SUB)
            nat[j, pl.ds(r, SUB, stride=steps), :] = fresh_ref[here, cols] + cum_a_ref[here, cols] * e
        path_ref[:, cols] = nat[j]


def norm_kernel(count, moves_ref, sums_ref, norm_ref, quad_ref):
    peers, tiles, _ = moves_ref.shape
    quad_ref[...] = jnp.zeros_like(quad_ref)

    def gather(q, carry):
        quad, sums = carry
        d = moves_ref[q]
        quad = quad + d * (sums_ref[q, 0:tiles, :] + sums_ref[q, tiles : 2 * tiles, :] * d)
        return quad, sums + sums_ref[q, 2 * tiles : 2 * tiles + SUB, :]

    quad, sums = lax.fori_loop(0, peers, gather, (quad_ref[0:tiles, :], quad_ref[tiles:, :]))
    extra = jnp.sum(quad, axis=0, keepdims=True)
    totals = [sums[0:1, :], sums[1:2, :], sums[2:3, :] + extra]
    for k, row in enumerate(totals):
        total = jnp.sum(row, axis=1, keepdims=True)
        norm_ref[k] = jnp.max(jnp.sqrt(total / count))


def exchange(pay):
    return lax.all_to_all(pay, "tm", 0, 0)


def body(gate_in, cand_in, rates, init_state, recur_weight):
    rows, width = gate_in.shape
    peers = lax.axis_size("tm")
    tiles = width // LANE
    steps = rows // SUB
    assert rows % (2 * SUB) == 0 and width % WIDE == 0
    me = lax.axis_index("tm").astype(jnp.int32).reshape(1)
    init_row = init_state.reshape(1, width)
    init_tile = init_state.reshape(tiles, LANE)
    vmem = pl.BlockSpec(memory_space=pltpu.VMEM)
    smem = pl.BlockSpec(memory_space=pltpu.SMEM)
    hbm = pl.BlockSpec(memory_space=pltpu.HBM)
    grid_f32 = jax.ShapeDtypeStruct((rows, width), F32)
    pay2 = jax.ShapeDtypeStruct((peers, 2 * tiles, LANE), F32)
    pay3 = jax.ShapeDtypeStruct((peers, 2 * tiles + SUB, LANE), F32)

    keep, base, cum_a, cum_b, diag, pay = pl.pallas_call(
        start_kernel,
        out_shape=(grid_f32, grid_f32, grid_f32, grid_f32, jax.ShapeDtypeStruct((1, width), F32), pay2),
        in_specs=[smem] + [hbm] * 5,
        out_specs=(vmem,) * 6,
        scratch_shapes=[
            pltpu.VMEM((rows, width), BF16),
            pltpu.VMEM((rows, width), BF16),
            pltpu.VMEM((1, width), F32),
            pltpu.VMEM((1, width), F32),
            pltpu.VMEM((width, width), BF16),
            pltpu.VMEM((tiles, LANE, LANE), BF16),
            pltpu.VMEM((tiles, rows, LANE), F32),
            pltpu.VMEM((tiles, rows, LANE), F32),
            pltpu.VMEM((1, width), F32),
            pltpu.VMEM((2 * tiles, LANE), F32),
            pltpu.SemaphoreType.DMA((2 * PARTS + 2,)),
            pltpu.SemaphoreType.DMA((PARTS,)),
            pltpu.SemaphoreType.DMA((tiles,)),
        ],
        compiler_params=pltpu.CompilerParams(vmem_limit_bytes=VMEM_LIMIT),
        name="start",
    )(me, *(pltpu.with_memory_space_constraint(x, pltpu.HBM) for x in (gate_in, cand_in, rates.reshape(1, width), init_row, recur_weight)))
    got = exchange(pay)

    scratch = [
        pltpu.VMEM((rows, width), F32),
        pltpu.VMEM((rows, width), BF16),
        pltpu.VMEM((tiles, LANE), F32),
    ]
    state, cum_a, cum_b, moved, pay = pl.pallas_call(
        first_step_kernel,
        out_shape=(grid_f32, grid_f32, grid_f32, jax.ShapeDtypeStruct((SUB, LANE), F32), pay2),
        in_specs=[smem] + [vmem] * 8,
        out_specs=(vmem,) * 5,
        scratch_shapes=scratch + [pltpu.VMEM((2 * tiles, LANE), F32), pltpu.VMEM((SUB, LANE), F32)],
        compiler_params=pltpu.CompilerParams(vmem_limit_bytes=VMEM_LIMIT),
        name="middle",
    )(me, got, init_tile, keep, base, cum_a, cum_b, diag, recur_weight)
    got = exchange(pay)

    fresh, cum_a, pay, sums = pl.pallas_call(
        functools.partial(step_kernel, True),
        out_shape=(grid_f32, grid_f32, pay2, pay3),
        in_specs=[smem] + [vmem] * 10,
        out_specs=(vmem,) * 4,
        scratch_shapes=scratch
        + [
            pltpu.VMEM((2 * tiles, LANE), F32),
            pltpu.VMEM((SUB, LANE), F32),
            pltpu.VMEM((2 * tiles + SUB, LANE), F32),
        ],
        compiler_params=pltpu.CompilerParams(vmem_limit_bytes=VMEM_LIMIT),
        name="last",
    )(me, got, init_tile, keep, base, cum_a, cum_b, diag, recur_weight, state, moved)
    got = exchange(pay)
    sums = exchange(sums)

    path, moves = pl.pallas_call(
        path_kernel,
        out_shape=(grid_f32, jax.ShapeDtypeStruct((peers, tiles, LANE), F32)),
        in_specs=[smem] + [vmem] * 3,
        out_specs=(vmem,) * 2,
        scratch_shapes=[pltpu.VMEM((tiles, rows, LANE), F32)],
        compiler_params=pltpu.CompilerParams(vmem_limit_bytes=VMEM_LIMIT),
        cost_estimate=pl.CostEstimate(flops=10**10, bytes_accessed=2**21, transcendentals=0),
        name="path",
    )(me, got, fresh, cum_a)
    norms = pl.pallas_call(
        functools.partial(norm_kernel, peers * rows * width),
        out_shape=jax.ShapeDtypeStruct((3,), F32),
        in_specs=[vmem] * 2,
        out_specs=smem,
        scratch_shapes=[pltpu.VMEM((tiles + SUB, LANE), F32)],
        compiler_params=pltpu.CompilerParams(vmem_limit_bytes=VMEM_LIMIT),
        name="norm",
    )(moves, sums)
    return path, norms


def solution(mesh):
    placed = (P("tm", "batch"), P("tm", "batch"), P("batch"), P("batch"), P())
    return jax.shard_map(
        body, mesh=mesh, in_specs=placed, out_specs=(P("tm", "batch"), P("batch")), check_vma=False
    )
```

```python
import functools

import jax
import jax.numpy as jnp
from jax import lax
from jax.experimental import pallas as pl
from jax.experimental.pallas import tpu as pltpu
from jax.sharding import PartitionSpec as P

SUB = 8
LANE = 128
WIDE = 256
PARTS = 4
VMEM_LIMIT = 16 * 1024 * 1024
F32 = jnp.float32
BF16 = jnp.bfloat16


def softplus(x):
    return jnp.maximum(x, 0.0) + jnp.log(1.0 + jnp.exp(-jnp.abs(x)))


def chunk_scan(mul, add):
    run_a, run_b = [mul[0]], [add[0]]
    for a, b in zip(mul[1:], add[1:]):
        run_a.append(a * run_a[-1])
        run_b.append(a * run_b[-1] + b)
    tot_a, tot_b = run_a[-1], run_b[-1]
    place = lax.broadcasted_iota(jnp.int32, tot_a.shape, 0)
    shift = 1
    while shift < SUB:
        far = place >= shift
        old_a = jnp.where(far, pltpu.roll(tot_a, shift, 0), 1.0)
        old_b = jnp.where(far, pltpu.roll(tot_b, shift, 0), 0.0)
        tot_b = tot_a * old_b + tot_b
        tot_a = tot_a * old_a
        shift *= 2
    far = place >= 1
    head_a = jnp.where(far, pltpu.roll(tot_a, 1, 0), 1.0)
    head_b = jnp.where(far, pltpu.roll(tot_b, 1, 0), 0.0)
    cum_a = [a * head_a for a in run_a]
    cum_b = [a * head_b + b for a, b in zip(run_a, run_b)]
    return cum_a, cum_b


def write_rows(ref, base, first_tile, row):
    for k in range(row.shape[1] // LANE):
        ref[pl.ds(base + first_tile + k, 1), :] = row[:, k * LANE : (k + 1) * LANE]


def read_row(ref, first_tile, tiles):
    return jnp.concatenate([ref[pl.ds(first_tile + k, 1), :] for k in range(tiles)], axis=1)


def spread(one_ref, out_ref):
    value = one_ref[...]
    for q in range(out_ref.shape[0]):
        out_ref[q] = value


def start_kernel(
    me_ref, gate_hbm, cand_hbm, rates_hbm, init_hbm, w_hbm,
    keep_ref, base_ref, cum_a_ref, cum_b_ref, diag_ref, pay_ref,
    gate_ref, cand_ref, rates_ref, init_ref, w_ref, blocks, gate_nat, base_nat, mixed, one,
    in_sem, w_sem, d_sem,
):
    rows, width = gate_ref.shape
    steps = rows // SUB
    tiles = width // LANE
    per = WIDE // LANE
    part = width // PARTS
    me = me_ref[0]

    def columns(hbm, ref, k, sem):
        cols = pl.ds(k * part, part)
        return pltpu.make_async_copy(hbm.at[:, cols], ref.at[:, cols], sem)

    rates_copy = pltpu.make_async_copy(rates_hbm, rates_ref, in_sem.at[2 * PARTS])
    init_copy = pltpu.make_async_copy(init_hbm, init_ref, in_sem.at[2 * PARTS + 1])
    gate_copies = [columns(gate_hbm, gate_ref, k, in_sem.at[k]) for k in range(PARTS)]
    cand_copies = [columns(cand_hbm, cand_ref, k, in_sem.at[PARTS + k]) for k in range(PARTS)]
    diag_copies = [
        pltpu.make_async_copy(
            w_hbm.at[pl.ds(k * LANE, LANE), pl.ds(k * LANE, LANE)], blocks.at[k], d_sem.at[k]
        )
        for k in range(tiles)
    ]
    w_copies = [
        pltpu.make_async_copy(
            w_hbm.at[pl.ds(k * part, part), :], w_ref.at[pl.ds(k * part, part), :], w_sem.at[k]
        )
        for k in range(PARTS)
    ]
    rates_copy.start()
    for k in range(PARTS):
        gate_copies[k].start()
        cand_copies[k].start()
    init_copy.start()
    for copy in diag_copies:
        copy.start()

    @pl.when(me == 0)
    def _():
        for copy in w_copies:
            copy.start()

    mixed[...] = jnp.zeros_like(mixed)
    rates_copy.wait()
    init_copy.wait()
    for copy in diag_copies:
        copy.wait()

    @pl.when(me == 0)
    def _():
        total = jnp.zeros((SUB, width), F32)
        for k in range(PARTS):
            w_copies[k].wait()
            left = jnp.broadcast_to(init_ref[:, k * part : (k + 1) * part], (SUB, part)).astype(BF16)
            total = total + jnp.dot(left, w_ref[k * part : (k + 1) * part, :], preferred_element_type=F32)
        mixed[...] = total[0:1, :]

    @pl.when(me != 0)
    def _():
        init_ref[...] = jnp.zeros_like(init_ref)

    turn = [pl.ds(r, SUB, stride=steps) for r in range(steps)]
    for p in range(PARTS):
        gate_copies[p].wait()
        cand_copies[p].wait()

        @pl.loop(p * (part // WIDE), (p + 1) * (part // WIDE))
        def _(j):
            cols = pl.ds(pl.multiple_of(j * WIDE, WIDE), WIDE)
            on_diag = lax.broadcasted_iota(jnp.int32, (LANE, LANE), 0) == lax.broadcasted_iota(
                jnp.int32, (LANE, LANE), 1
            )
            units = []
            for k in range(per):
                here = pl.ds(pl.multiple_of(j * WIDE + k * LANE, LANE), LANE)
                gate_nat[j * per + k] = gate_ref[:, here].astype(F32)
                base_nat[j * per + k] = cand_ref[:, here].astype(F32)
                block = jnp.where(on_diag, blocks[j * per + k].astype(F32), 0.0)
                units.append(jnp.sum(block, axis=0, keepdims=True))
            unit = jnp.concatenate(units, axis=1)
            diag_ref[:, cols] = unit
            top = lax.broadcasted_iota(jnp.int32, (SUB, WIDE), 0) == 0
            rate = rates_ref[:, cols]
            mul, add = [], []
            for r in range(steps):
                here = pl.ds(r * SUB, SUB)
                gate = jnp.concatenate([gate_nat[j * per + k, turn[r], :] for k in range(per)], axis=1)
                base = jnp.concatenate([base_nat[j * per + k, turn[r], :] for k in range(per)], axis=1)
                keep = jnp.exp(-rate * softplus(gate) - jnp.maximum(gate - 8.0, 0.0))
                keep_ref[here, cols] = keep
                base_ref[here, cols] = base
                left = 1.0 - keep
                cand = jnp.tanh(base + jnp.where(top, mixed[:, cols], 0.0) if r == 0 else base)
                slope = keep + left * (1.0 - cand * cand) * unit
                offset = left * cand
                if r == 0:
                    prev = jnp.where(top, init_ref[:, cols], 0.0)
                    offset = (keep * prev + offset) - slope * prev
                mul.append(slope)
                add.append(offset)
            cum_a, cum_b = chunk_scan(mul, add)
            for r in range(steps):
                here = pl.ds(r * SUB, SUB)
                cum_a_ref[here, cols] = cum_a[r]
                cum_b_ref[here, cols] = cum_b[r]
            write_rows(one, 0, j * per, cum_a[-1][SUB - 1 :, :])
            write_rows(one, tiles, j * per, cum_b[-1][SUB - 1 :, :])

    spread(one, pay_ref)


def step_kernel(
    last, me_ref, got_ref, init_ref, keep_ref, base_ref, cum_a_ref, cum_b_ref, diag_ref, w_ref, old_ref, tot_ref,
    *rest,
):
    if last:
        fresh_ref, out_a_ref, one, prev, low, entry, acc, mix = rest
    else:
        state_ref, out_a_ref, out_b_ref, sum_ref, pay_ref, prev, low, entry, one, acc, mix = rest
    rows, width = keep_ref.shape
    steps = rows // SUB
    tiles = width // LANE
    per = WIDE // LANE

    def pull(q, e):
        return got_ref[q, 0:tiles, :] * e + got_ref[q, tiles : 2 * tiles, :]

    entry[...] = lax.fori_loop(0, me_ref[0], pull, init_ref[...])
    acc[...] = jnp.zeros_like(acc)

    def turned_state(j, _):
        cols = pl.ds(pl.multiple_of(j * WIDE, WIDE), WIDE)
        e = read_row(entry, j * per, per)
        state = [
            cum_b_ref[pl.ds(r * SUB, SUB), cols] + cum_a_ref[pl.ds(r * SUB, SUB), cols] * e for r in range(steps)
        ]
        place = lax.broadcasted_iota(jnp.int32, state[0].shape, 0)
        before = [jnp.where(place == 0, jnp.broadcast_to(e, state[0].shape), pltpu.roll(state[-1], 1, 0))] + state[:-1]
        moved = 0.0
        for r in range(steps):
            prev[pl.ds(r * SUB, SUB), cols] = before[r]
            change = state[r] if old_ref is None else state[r] - old_ref[pl.ds(r * SUB, SUB), cols]
            moved = moved + change * change
            if not last:
                state_ref[pl.ds(r * SUB, SUB), cols] = state[r]
        for r in range(0, steps, 2):
            low[pl.ds(r * SUB, 2 * SUB), cols] = jnp.concatenate(before[r : r + 2], axis=0).astype(BF16)
        acc[...] += sum(moved[:, k * LANE : (k + 1) * LANE] for k in range(per))
        return 0

    lax.fori_loop(0, width // WIDE, turned_state, 0)
    if not last:
        sum_ref[...] = acc[...]
    else:
        one[pl.ds(4 * tiles, SUB), :] = jnp.zeros((SUB, LANE), F32)
        one[pl.ds(4 * tiles, 1), :] = jnp.sum(tot_ref[...], axis=0, keepdims=True)
        one[pl.ds(4 * tiles + 1, 1), :] = jnp.sum(acc[...], axis=0, keepdims=True)
        acc[...] = jnp.zeros_like(acc)

    def multiply(j, slot):
        cols = pl.ds(pl.multiple_of(j * WIDE, WIDE), WIDE)
        mix[slot] = jnp.dot(low[...], w_ref[:, cols], preferred_element_type=F32)

    def solve(j, slot):
        cols = pl.ds(pl.multiple_of(j * WIDE, WIDE), WIDE)
        unit = diag_ref[:, cols]
        mul, add = [], []
        for r in range(steps):
            here = pl.ds(r * SUB, SUB)
            keep = keep_ref[here, cols]
            before = prev[here, cols]
            cand = jnp.tanh(base_ref[here, cols] + mix[slot, here, :])
            left = 1.0 - keep
            mapped = keep * before + left * cand
            slope = keep + left * (1.0 - cand * cand) * unit
            mul.append(slope)
            add.append(mapped - slope * before)
        cum_a, cum_b = chunk_scan(mul, add)
        if last:
            e = read_row(entry, j * per, per)
            c0, c1, c2 = 0.0, 0.0, 0.0
            for r in range(steps):
                here = pl.ds(r * SUB, SUB)
                fresh = cum_b[r] + cum_a[r] * e
                if r + 1 < steps:
                    state = prev[pl.ds((r + 1) * SUB, SUB), cols]
                else:
                    state = cum_b_ref[here, cols] + cum_a_ref[here, cols] * e
                u = fresh - state
                for k in range(per):
                    part = slice(k * LANE, (k + 1) * LANE)
                    fresh_ref[j * per + k, pl.ds(r, SUB, stride=steps), :] = fresh[:, part]
                    out_a_ref[j * per + k, pl.ds(r, SUB, stride=steps), :] = cum_a[r][:, part]
                c0 = c0 + u * u
                c1 = c1 + u * cum_a[r]
                c2 = c2 + cum_a[r] * cum_a[r]
            acc[...] += sum(c0[:, k * LANE : (k + 1) * LANE] for k in range(per))
            write_rows(one, 0, j * per, cum_a[-1][SUB - 1 :, :])
            write_rows(one, tiles, j * per, u[SUB - 1 :, :])
            write_rows(one, 2 * tiles, j * per, 2.0 * jnp.sum(c1, axis=0, keepdims=True))
            write_rows(one, 3 * tiles, j * per, jnp.sum(c2, axis=0, keepdims=True))
        else:
            for r in range(steps):
                here = pl.ds(r * SUB, SUB)
                out_a_ref[here, cols] = cum_a[r]
                out_b_ref[here, cols] = cum_b[r]
            write_rows(one, 0, j * per, cum_a[-1][SUB - 1 :, :])
            write_rows(one, tiles, j * per, cum_b[-1][SUB - 1 :, :])

    blocks = width // WIDE
    multiply(0, 0)

    @pl.loop(0, blocks // 2 - 1)
    def _(i):
        multiply(2 * i + 1, 1)
        solve(2 * i, 0)
        multiply(2 * i + 2, 0)
        solve(2 * i + 1, 1)

    multiply(blocks - 1, 1)
    solve(blocks - 2, 0)
    solve(blocks - 1, 1)
    if last:
        one[pl.ds(4 * tiles + 2, 1), :] = jnp.sum(acc[...], axis=0, keepdims=True)
    else:
        spread(one, pay_ref)


def first_step_kernel(me, got, init, keep, base, cum_a, cum_b, diag, w, *rest):
    step_kernel(False, me, got, init, keep, base, cum_a, cum_b, diag, w, None, None, *rest)


def pair_kernel(me_ref, one_ref, other_ref, pay_ref, both):
    tiles = (one_ref.shape[0] - SUB) // 4

    def join(first, second):
        a1, b1, l1, q1 = (first[k * tiles : (k + 1) * tiles, :] for k in range(4))
        a2, b2, l2, q2 = (second[k * tiles : (k + 1) * tiles, :] for k in range(4))
        both[0:tiles, :] = a1 * a2
        both[tiles : 2 * tiles, :] = a2 * b1 + b2
        both[2 * tiles : 3 * tiles, :] = l1 + a1 * (l2 + 2.0 * q2 * b1)
        both[3 * tiles : 4 * tiles, :] = q1 + a1 * a1 * q2
        both[4 * tiles :, :] = first[4 * tiles :, :] + second[4 * tiles :, :]
        extra = jnp.sum(b1 * (l2 + q2 * b1), axis=0, keepdims=True)
        both[4 * tiles + 2 : 4 * tiles + 3, :] = both[4 * tiles + 2 : 4 * tiles + 3, :] + extra

    @pl.when(lax.rem(me_ref[0], 2) == 0)
    def _():
        join(one_ref, other_ref)

    @pl.when(lax.rem(me_ref[0], 2) == 1)
    def _():
        join(other_ref, one_ref)

    spread(both, pay_ref)


def final_kernel(count, me_ref, got_ref, other_ref, fresh_ref, cum_a_ref, path_ref, norm_ref, entry, quad_ref):
    tiles = fresh_ref.shape[0]
    pairs = got_ref.shape[0]
    quad_ref[...] = jnp.zeros_like(quad_ref)
    pair = lax.div(me_ref[0], 2)

    def pull(q, carry):
        d, quad, sums = carry

        @pl.when(q == pair)
        def _():
            entry[...] = d

        quad = quad + d * (got_ref[q, 2 * tiles : 3 * tiles, :] + got_ref[q, 3 * tiles : 4 * tiles, :] * d)
        sums = sums + got_ref[q, 4 * tiles : 4 * tiles + SUB, :]
        return got_ref[q, 0:tiles, :] * d + got_ref[q, tiles : 2 * tiles, :], quad, sums

    _, quad, sums = lax.fori_loop(
        0, pairs, pull, (quad_ref[0:tiles, :], quad_ref[0:tiles, :], quad_ref[tiles:, :])
    )

    @pl.when(lax.rem(me_ref[0], 2) == 1)
    def _():
        entry[...] = other_ref[0:tiles, :] * entry[...] + other_ref[tiles : 2 * tiles, :]

    extra = jnp.sum(quad, axis=0, keepdims=True)
    totals = [sums[0:1, :], sums[1:2, :], sums[2:3, :] + extra]
    for k, row in enumerate(totals):
        total = jnp.sum(row, axis=1, keepdims=True)
        norm_ref[k] = jnp.max(jnp.sqrt(total / count))

    @pl.loop(0, tiles)
    def _(j):
        cols = pl.ds(pl.multiple_of(j * LANE, LANE), LANE)
        path_ref[:, cols] = fresh_ref[j] + cum_a_ref[j] * entry[pl.ds(j, 1), :]


def exchange(pay, groups=None):
    return lax.all_to_all(pay, "tm", 0, 0, axis_index_groups=groups)


def body(gate_in, cand_in, rates, init_state, recur_weight):
    rows, width = gate_in.shape
    peers = lax.axis_size("tm")
    tiles = width // LANE
    steps = rows // SUB
    assert rows % (2 * SUB) == 0 and width % (2 * WIDE) == 0 and peers % 2 == 0
    me = lax.axis_index("tm").astype(jnp.int32).reshape(1)
    init_row = init_state.reshape(1, width)
    init_tile = init_state.reshape(tiles, LANE)
    vmem = pl.BlockSpec(memory_space=pltpu.VMEM)
    smem = pl.BlockSpec(memory_space=pltpu.SMEM)
    hbm = pl.BlockSpec(memory_space=pltpu.HBM)
    grid_f32 = jax.ShapeDtypeStruct((rows, width), F32)
    pay2 = jax.ShapeDtypeStruct((peers, 2 * tiles, LANE), F32)
    last1 = jax.ShapeDtypeStruct((4 * tiles + SUB, LANE), F32)
    last8 = jax.ShapeDtypeStruct((peers // 2, 4 * tiles + SUB, LANE), F32)
    turned = jax.ShapeDtypeStruct((tiles, rows, LANE), F32)

    keep, base, cum_a, cum_b, diag, pay = pl.pallas_call(
        start_kernel,
        out_shape=(grid_f32, grid_f32, grid_f32, grid_f32, jax.ShapeDtypeStruct((1, width), F32), pay2),
        in_specs=[smem] + [hbm] * 5,
        out_specs=(vmem,) * 6,
        scratch_shapes=[
            pltpu.VMEM((rows, width), BF16),
            pltpu.VMEM((rows, width), BF16),
            pltpu.VMEM((1, width), F32),
            pltpu.VMEM((1, width), F32),
            pltpu.VMEM((width, width), BF16),
            pltpu.VMEM((tiles, LANE, LANE), BF16),
            pltpu.VMEM((tiles, rows, LANE), F32),
            pltpu.VMEM((tiles, rows, LANE), F32),
            pltpu.VMEM((1, width), F32),
            pltpu.VMEM((2 * tiles, LANE), F32),
            pltpu.SemaphoreType.DMA((2 * PARTS + 2,)),
            pltpu.SemaphoreType.DMA((PARTS,)),
            pltpu.SemaphoreType.DMA((tiles,)),
        ],
        compiler_params=pltpu.CompilerParams(vmem_limit_bytes=VMEM_LIMIT),
        name="start",
    )(me, *(pltpu.with_memory_space_constraint(x, pltpu.HBM) for x in (gate_in, cand_in, rates.reshape(1, width), init_row, recur_weight)))
    got = exchange(pay)

    scratch = [
        pltpu.VMEM((rows, width), F32),
        pltpu.VMEM((rows, width), BF16),
        pltpu.VMEM((tiles, LANE), F32),
    ]
    tail = [pltpu.VMEM((SUB, LANE), F32), pltpu.VMEM((2, rows, WIDE), F32)]
    state, cum_a, cum_b, moved, pay = pl.pallas_call(
        first_step_kernel,
        out_shape=(grid_f32, grid_f32, grid_f32, jax.ShapeDtypeStruct((SUB, LANE), F32), pay2),
        in_specs=[smem] + [vmem] * 8,
        out_specs=(vmem,) * 5,
        scratch_shapes=scratch + [pltpu.VMEM((2 * tiles, LANE), F32)] + tail,
        compiler_params=pltpu.CompilerParams(vmem_limit_bytes=VMEM_LIMIT),
        name="middle",
    )(me, got, init_tile, keep, base, cum_a, cum_b, diag, recur_weight)
    got = exchange(pay)

    fresh, cum_a, one = pl.pallas_call(
        functools.partial(step_kernel, True),
        out_shape=(turned, turned, last1),
        in_specs=[smem] + [vmem] * 10,
        out_specs=(vmem,) * 3,
        scratch_shapes=scratch + tail,
        compiler_params=pltpu.CompilerParams(vmem_limit_bytes=VMEM_LIMIT),
        name="last",
    )(me, got, init_tile, keep, base, cum_a, cum_b, diag, recur_weight, state, moved)

    other = lax.ppermute(one, "tm", [(k, k ^ 1) for k in range(peers)])
    pay = pl.pallas_call(
        pair_kernel,
        out_shape=last8,
        in_specs=[smem] + [vmem] * 2,
        out_specs=vmem,
        scratch_shapes=[pltpu.VMEM(last1.shape, F32)],
        compiler_params=pltpu.CompilerParams(vmem_limit_bytes=VMEM_LIMIT),
        name="pair",
    )(me, one, other)
    got = exchange(pay, [[2 * k + s for k in range(peers // 2)] for s in range(2)])

    path, norms = pl.pallas_call(
        functools.partial(final_kernel, peers * rows * width),
        out_shape=(grid_f32, jax.ShapeDtypeStruct((3,), F32)),
        in_specs=[smem] + [vmem] * 4,
        out_specs=(vmem, smem),
        scratch_shapes=[pltpu.VMEM((tiles, LANE), F32), pltpu.VMEM((tiles + SUB, LANE), F32)],
        compiler_params=pltpu.CompilerParams(vmem_limit_bytes=VMEM_LIMIT),
        name="final",
    )(me, got, other, fresh, cum_a)
    return path, norms


def solution(mesh):
    placed = (P("tm", "batch"), P("tm", "batch"), P("batch"), P("batch"), P())
    return jax.shard_map(
        body, mesh=mesh, in_specs=placed, out_specs=(P("tm", "batch"), P("batch")), check_vma=False
    )
```

```python
import functools

import jax
import jax.numpy as jnp
from jax import lax
from jax.experimental import pallas as pl
from jax.experimental.pallas import tpu as pltpu
from jax.sharding import PartitionSpec as P

SUB = 8
LANE = 128
WIDE = 256
PARTS = 2
CHUNKS = 2
VMEM_LIMIT = 16 * 1024 * 1024
F32 = jnp.float32
BF16 = jnp.bfloat16


LOG2E = 1.4426950408889634


def keep_of(gate, rate2):
    soft = jnp.maximum(gate, 0.0) + jnp.log(1.0 + jnp.exp2(jnp.abs(gate) * -LOG2E))
    return jnp.exp2(-rate2 * soft - jnp.maximum(gate * LOG2E - 8.0 * LOG2E, 0.0))


def chunk_scan(mul, add):
    run_a, run_b = [mul[0]], [add[0]]
    for a, b in zip(mul[1:], add[1:]):
        run_a.append(a * run_a[-1])
        run_b.append(a * run_b[-1] + b)
    tot_a, tot_b = run_a[-1], run_b[-1]
    place = lax.broadcasted_iota(jnp.int32, tot_a.shape, 0)
    shift = 1
    while shift < SUB:
        far = place >= shift
        old_a = jnp.where(far, pltpu.roll(tot_a, shift, 0), 1.0)
        old_b = jnp.where(far, pltpu.roll(tot_b, shift, 0), 0.0)
        tot_b = tot_a * old_b + tot_b
        tot_a = tot_a * old_a
        shift *= 2
    far = place >= 1
    head_a = jnp.where(far, pltpu.roll(tot_a, 1, 0), 1.0)
    head_b = jnp.where(far, pltpu.roll(tot_b, 1, 0), 0.0)
    cum_a = [a * head_a for a in run_a]
    cum_b = [a * head_b + b for a, b in zip(run_a, run_b)]
    return cum_a, cum_b


def write_rows(ref, base, first_tile, row):
    for k in range(row.shape[1] // LANE):
        ref[pl.ds(base + first_tile + k, 1), :] = row[:, k * LANE : (k + 1) * LANE]


def read_row(ref, first_tile, tiles):
    return jnp.concatenate([ref[pl.ds(first_tile + k, 1), :] for k in range(tiles)], axis=1)


def spread(one_ref, out_ref):
    value = one_ref[...]
    for q in range(out_ref.shape[0]):
        out_ref[q] = value


def start_kernel(
    me_ref, gate_hbm, cand_hbm, rates_hbm, init_hbm, w_hbm,
    keep_ref, base_ref, cum_a_ref, cum_b_ref, diag_ref, pay_ref,
    gate_ref, cand_ref, rates_ref, init_ref, w_ref, blocks, gate_nat, base_nat, mixed, one,
    in_sem, w_sem, d_sem,
):
    rows, width = gate_ref.shape
    steps = rows // SUB
    tiles = width // LANE
    per = WIDE // LANE
    part = width // PARTS
    me = me_ref[0]

    def columns(hbm, ref, k, sem):
        cols = pl.ds(k * part, part)
        return pltpu.make_async_copy(hbm.at[:, cols], ref.at[:, cols], sem)

    rates_copy = pltpu.make_async_copy(rates_hbm, rates_ref, in_sem.at[2 * PARTS])
    init_copy = pltpu.make_async_copy(init_hbm, init_ref, in_sem.at[2 * PARTS + 1])
    gate_copies = [columns(gate_hbm, gate_ref, k, in_sem.at[k]) for k in range(PARTS)]
    cand_copies = [columns(cand_hbm, cand_ref, k, in_sem.at[PARTS + k]) for k in range(PARTS)]
    diag_copies = [
        pltpu.make_async_copy(
            w_hbm.at[pl.ds(k * LANE, LANE), pl.ds(k * LANE, LANE)], blocks.at[k], d_sem.at[k]
        )
        for k in range(tiles)
    ]
    w_copies = [
        pltpu.make_async_copy(
            w_hbm.at[pl.ds(k * part, part), :], w_ref.at[pl.ds(k * part, part), :], w_sem.at[k]
        )
        for k in range(PARTS)
    ]
    for k in range(PARTS):
        gate_copies[k].start()
        cand_copies[k].start()
    rates_copy.start()
    init_copy.start()
    for copy in diag_copies:
        copy.start()

    @pl.when(me == 0)
    def _():
        for copy in w_copies:
            copy.start()

    mixed[...] = jnp.zeros_like(mixed)
    rates_copy.wait()
    init_copy.wait()
    for copy in diag_copies:
        copy.wait()

    @pl.when(me == 0)
    def _():
        total = jnp.zeros((SUB, width), F32)
        for k in range(PARTS):
            w_copies[k].wait()
            left = jnp.broadcast_to(init_ref[:, k * part : (k + 1) * part], (SUB, part)).astype(BF16)
            total = total + jnp.dot(left, w_ref[k * part : (k + 1) * part, :], preferred_element_type=F32)
        mixed[...] = total[0:1, :]

    @pl.when(me != 0)
    def _():
        init_ref[...] = jnp.zeros_like(init_ref)

    turn = [pl.ds(r, SUB, stride=steps) for r in range(steps)]
    for p in range(PARTS):
        gate_copies[p].wait()
        cand_copies[p].wait()

        @pl.loop(p * (part // WIDE), (p + 1) * (part // WIDE), unroll=True)
        def _(j):
            cols = pl.ds(pl.multiple_of(j * WIDE, WIDE), WIDE)
            on_diag = lax.broadcasted_iota(jnp.int32, (LANE, LANE), 0) == lax.broadcasted_iota(
                jnp.int32, (LANE, LANE), 1
            )
            units = []
            for k in range(per):
                here = pl.ds(pl.multiple_of(j * WIDE + k * LANE, LANE), LANE)
                gate_nat[j * per + k] = gate_ref[:, here].astype(F32)
                base_nat[j * per + k] = cand_ref[:, here].astype(F32)
                block = jnp.where(on_diag, blocks[j * per + k].astype(F32), 0.0)
                units.append(jnp.sum(block, axis=0, keepdims=True))
            unit = jnp.concatenate(units, axis=1)
            diag_ref[:, cols] = unit
            top = lax.broadcasted_iota(jnp.int32, (SUB, WIDE), 0) == 0
            rate = rates_ref[:, cols] * LOG2E
            mul, add = [], []
            for r in range(steps):
                here = pl.ds(r * SUB, SUB)
                gate = jnp.concatenate([gate_nat[j * per + k, turn[r], :] for k in range(per)], axis=1)
                base = jnp.concatenate([base_nat[j * per + k, turn[r], :] for k in range(per)], axis=1)
                keep = keep_of(gate, rate)
                keep_ref[here, cols] = keep
                base_ref[here, cols] = base
                left = 1.0 - keep
                cand = jnp.tanh(base + jnp.where(top, mixed[:, cols], 0.0) if r == 0 else base)
                slope = keep + left * (1.0 - cand * cand) * unit
                offset = left * cand
                if r == 0:
                    prev = jnp.where(top, init_ref[:, cols], 0.0)
                    offset = (keep * prev + offset) - slope * prev
                mul.append(slope)
                add.append(offset)
            cum_a, cum_b = chunk_scan(mul, add)
            for r in range(steps):
                here = pl.ds(r * SUB, SUB)
                cum_a_ref[here, cols] = cum_a[r]
                cum_b_ref[here, cols] = cum_b[r]
            write_rows(one, 0, j * per, cum_a[-1][SUB - 1 :, :])
            write_rows(one, tiles, j * per, cum_b[-1][SUB - 1 :, :])

    spread(one, pay_ref)


def step_kernel(
    last, me_ref, got_ref, init_ref, keep_ref, base_ref, cum_a_ref, cum_b_ref, diag_ref, w_ref, old_ref, tot_ref,
    *rest,
):
    if last:
        fresh_ref, out_a_ref, one, prev, low, entry, acc, mix = rest
    else:
        state_ref, out_a_ref, out_b_ref, sum_ref, pay_ref, prev, low, entry, one, acc, mix = rest
    rows, width = keep_ref.shape
    steps = rows // SUB
    tiles = width // LANE
    per = WIDE // LANE

    def pull(q, e):
        return got_ref[q, 0:tiles, :] * e + got_ref[q, tiles : 2 * tiles, :]

    entry[...] = lax.fori_loop(0, me_ref[0], pull, init_ref[...])
    acc[...] = jnp.zeros_like(acc)

    def turned_state(j):
        cols = slice(j * WIDE, (j + 1) * WIDE)
        e = read_row(entry, j * per, per)
        state = [
            cum_b_ref[pl.ds(r * SUB, SUB), cols] + cum_a_ref[pl.ds(r * SUB, SUB), cols] * e for r in range(steps)
        ]
        place = lax.broadcasted_iota(jnp.int32, state[0].shape, 0)
        before = [jnp.where(place == 0, jnp.broadcast_to(e, state[0].shape), pltpu.roll(state[-1], 1, 0))] + state[:-1]
        moved = 0.0
        for r in range(steps):
            prev[pl.ds(r * SUB, SUB), cols] = before[r]
            change = state[r] if old_ref is None else state[r] - old_ref[pl.ds(r * SUB, SUB), cols]
            moved = moved + change * change
            if not last:
                state_ref[pl.ds(r * SUB, SUB), cols] = state[r]
        rounded = jnp.concatenate(before, axis=0).astype(BF16)
        low[:, cols] = rounded
        acc[...] += sum(moved[:, k * LANE : (k + 1) * LANE] for k in range(per))
        return jnp.dot(rounded, w_ref[cols, 0:WIDE], preferred_element_type=F32)

    mix[0] = sum(turned_state(j) for j in range(width // WIDE))
    if not last:
        sum_ref[...] = acc[...]
    else:
        one[pl.ds(4 * tiles, SUB), :] = jnp.zeros((SUB, LANE), F32)
        one[pl.ds(4 * tiles, 1), :] = jnp.sum(tot_ref[...], axis=0, keepdims=True)
        one[pl.ds(4 * tiles + 1, 1), :] = jnp.sum(acc[...], axis=0, keepdims=True)
        acc[...] = jnp.zeros_like(acc)

    def multiply(j, slot):
        cols = pl.ds(pl.multiple_of(j * WIDE, WIDE), WIDE)
        mix[slot] = jnp.dot(low[...], w_ref[:, cols], preferred_element_type=F32)

    def solve(j, slot):
        cols = pl.ds(pl.multiple_of(j * WIDE, WIDE), WIDE)
        unit = diag_ref[:, cols]
        mul, add = [], []
        for r in range(steps):
            here = pl.ds(r * SUB, SUB)
            keep = keep_ref[here, cols]
            before = prev[here, cols]
            cand = jnp.tanh(base_ref[here, cols] + mix[slot, here, :])
            left = 1.0 - keep
            mapped = keep * before + left * cand
            slope = keep + left * (1.0 - cand * cand) * unit
            mul.append(slope)
            add.append(mapped - slope * before)
        cum_a, cum_b = chunk_scan(mul, add)
        if last:
            e = read_row(entry, j * per, per)
            c0, c1, c2 = 0.0, 0.0, 0.0
            for r in range(steps):
                here = pl.ds(r * SUB, SUB)
                fresh = cum_b[r] + cum_a[r] * e
                if r + 1 < steps:
                    state = prev[pl.ds((r + 1) * SUB, SUB), cols]
                else:
                    state = cum_b_ref[here, cols] + cum_a_ref[here, cols] * e
                u = fresh - state
                for k in range(per):
                    part = slice(k * LANE, (k + 1) * LANE)
                    fresh_ref[j * per + k, pl.ds(r, SUB, stride=steps), :] = fresh[:, part]
                    out_a_ref[j * per + k, pl.ds(r, SUB, stride=steps), :] = cum_a[r][:, part]
                c0 = c0 + u * u
                c1 = c1 + u * cum_a[r]
                c2 = c2 + cum_a[r] * cum_a[r]
            acc[...] += sum(c0[:, k * LANE : (k + 1) * LANE] for k in range(per))
            write_rows(one, 0, j * per, cum_a[-1][SUB - 1 :, :])
            write_rows(one, tiles, j * per, u[SUB - 1 :, :])
            write_rows(one, 2 * tiles, j * per, 2.0 * jnp.sum(c1, axis=0, keepdims=True))
            write_rows(one, 3 * tiles, j * per, jnp.sum(c2, axis=0, keepdims=True))
        else:
            for r in range(steps):
                here = pl.ds(r * SUB, SUB)
                out_a_ref[here, cols] = cum_a[r]
                out_b_ref[here, cols] = cum_b[r]
            write_rows(one, 0, j * per, cum_a[-1][SUB - 1 :, :])
            write_rows(one, tiles, j * per, cum_b[-1][SUB - 1 :, :])

    blocks = width // WIDE

    @pl.loop(0, blocks // 2 - 1, unroll=True)
    def _(i):
        multiply(2 * i + 1, 1)
        solve(2 * i, 0)
        multiply(2 * i + 2, 0)
        solve(2 * i + 1, 1)

    multiply(blocks - 1, 1)
    solve(blocks - 2, 0)
    solve(blocks - 1, 1)
    if last:
        one[pl.ds(4 * tiles + 2, 1), :] = jnp.sum(acc[...], axis=0, keepdims=True)
    else:
        spread(one, pay_ref)


def first_step_kernel(me, got, init, keep, base, cum_a, cum_b, diag, w, *rest):
    step_kernel(False, me, got, init, keep, base, cum_a, cum_b, diag, w, None, None, *rest)


def pair_kernel(me_ref, one_ref, other_ref, pay_ref, both):
    tiles = (one_ref.shape[0] - SUB) // 4

    def join(first, second):
        a1, b1, l1, q1 = (first[k * tiles : (k + 1) * tiles, :] for k in range(4))
        a2, b2, l2, q2 = (second[k * tiles : (k + 1) * tiles, :] for k in range(4))
        both[0:tiles, :] = a1 * a2
        both[tiles : 2 * tiles, :] = a2 * b1 + b2
        both[2 * tiles : 3 * tiles, :] = l1 + a1 * (l2 + 2.0 * q2 * b1)
        both[3 * tiles : 4 * tiles, :] = q1 + a1 * a1 * q2
        both[4 * tiles :, :] = first[4 * tiles :, :] + second[4 * tiles :, :]
        extra = jnp.sum(b1 * (l2 + q2 * b1), axis=0, keepdims=True)
        both[4 * tiles + 2 : 4 * tiles + 3, :] = both[4 * tiles + 2 : 4 * tiles + 3, :] + extra

    @pl.when(lax.rem(me_ref[0], 2) == 0)
    def _():
        join(one_ref, other_ref)

    @pl.when(lax.rem(me_ref[0], 2) == 1)
    def _():
        join(other_ref, one_ref)

    spread(both, pay_ref)


def final_kernel(
    count, me_ref, got_ref, other_ref, fresh_ref, cum_a_ref, path_hbm, norm_hbm, moves, entry, path, norm_ref, sem
):
    tiles, rows, _ = fresh_ref.shape
    pairs = got_ref.shape[0]
    moves[0] = jnp.zeros((tiles, LANE), F32)

    def pull(q, d):
        d = got_ref[q, 0:tiles, :] * d + got_ref[q, tiles : 2 * tiles, :]
        moves[q + 1] = d
        return d

    lax.fori_loop(0, pairs - 1, pull, moves[0], unroll=True)
    entry[...] = moves[lax.div(me_ref[0], 2)]

    @pl.when(lax.rem(me_ref[0], 2) == 1)
    def _():
        entry[...] = other_ref[0:tiles, :] * entry[...] + other_ref[tiles : 2 * tiles, :]

    copies = []
    for p in range(CHUNKS):
        for j in range(p * tiles // CHUNKS, (p + 1) * tiles // CHUNKS):
            path[:, j * LANE : (j + 1) * LANE] = fresh_ref[j] + cum_a_ref[j] * entry[j : j + 1, :]
        here = pl.ds(p * (tiles // CHUNKS) * LANE, (tiles // CHUNKS) * LANE)
        copies.append(pltpu.make_async_copy(path.at[:, here], path_hbm.at[:, here], sem.at[p]))
        copies[-1].start()

    def gather(q, carry):
        quad, sums = carry
        d = moves[q]
        quad = quad + d * (got_ref[q, 2 * tiles : 3 * tiles, :] + got_ref[q, 3 * tiles : 4 * tiles, :] * d)
        return quad, sums + got_ref[q, 4 * tiles : 4 * tiles + SUB, :]

    quad, sums = lax.fori_loop(0, pairs, gather, (moves[0], moves[0, 0:SUB, :]), unroll=True)
    extra = jnp.sum(quad, axis=0, keepdims=True)
    totals = [sums[0:1, :], sums[1:2, :], sums[2:3, :] + extra]
    for k, row in enumerate(totals):
        total = jnp.sum(row, axis=1, keepdims=True)
        norm_ref[k] = jnp.max(jnp.sqrt(total / count))
    copies.append(pltpu.make_async_copy(norm_ref, norm_hbm, sem.at[CHUNKS]))
    copies[-1].start()
    for copy in copies:
        copy.wait()


def exchange(pay, groups=None):
    return lax.all_to_all(pay, "tm", 0, 0, axis_index_groups=groups)


def body(gate_in, cand_in, rates, init_state, recur_weight):
    rows, width = gate_in.shape
    peers = lax.axis_size("tm")
    tiles = width // LANE
    steps = rows // SUB
    assert rows % (2 * SUB) == 0 and width % (2 * WIDE) == 0 and peers % 2 == 0
    me = lax.axis_index("tm").astype(jnp.int32).reshape(1)
    init_row = init_state.reshape(1, width)
    init_tile = init_state.reshape(tiles, LANE)
    vmem = pl.BlockSpec(memory_space=pltpu.VMEM)
    smem = pl.BlockSpec(memory_space=pltpu.SMEM)
    hbm = pl.BlockSpec(memory_space=pltpu.HBM)
    grid_f32 = jax.ShapeDtypeStruct((rows, width), F32)
    pay2 = jax.ShapeDtypeStruct((peers, 2 * tiles, LANE), F32)
    last1 = jax.ShapeDtypeStruct((4 * tiles + SUB, LANE), F32)
    last8 = jax.ShapeDtypeStruct((peers // 2, 4 * tiles + SUB, LANE), F32)
    turned = jax.ShapeDtypeStruct((tiles, rows, LANE), F32)

    keep, base, cum_a, cum_b, diag, pay = pl.pallas_call(
        start_kernel,
        out_shape=(grid_f32, grid_f32, grid_f32, grid_f32, jax.ShapeDtypeStruct((1, width), F32), pay2),
        in_specs=[smem] + [hbm] * 5,
        out_specs=(vmem,) * 6,
        scratch_shapes=[
            pltpu.VMEM((rows, width), BF16),
            pltpu.VMEM((rows, width), BF16),
            pltpu.VMEM((1, width), F32),
            pltpu.VMEM((1, width), F32),
            pltpu.VMEM((width, width), BF16),
            pltpu.VMEM((tiles, LANE, LANE), BF16),
            pltpu.VMEM((tiles, rows, LANE), F32),
            pltpu.VMEM((tiles, rows, LANE), F32),
            pltpu.VMEM((1, width), F32),
            pltpu.VMEM((2 * tiles, LANE), F32),
            pltpu.SemaphoreType.DMA((2 * PARTS + 2,)),
            pltpu.SemaphoreType.DMA((PARTS,)),
            pltpu.SemaphoreType.DMA((tiles,)),
        ],
        compiler_params=pltpu.CompilerParams(vmem_limit_bytes=VMEM_LIMIT),
        name="start",
    )(me, *(pltpu.with_memory_space_constraint(x, pltpu.HBM) for x in (gate_in, cand_in, rates.reshape(1, width), init_row, recur_weight)))
    got = exchange(pay)

    scratch = [
        pltpu.VMEM((rows, width), F32),
        pltpu.VMEM((rows, width), BF16),
        pltpu.VMEM((tiles, LANE), F32),
    ]
    tail = [pltpu.VMEM((SUB, LANE), F32), pltpu.VMEM((2, rows, WIDE), F32)]
    state, cum_a, cum_b, moved, pay = pl.pallas_call(
        first_step_kernel,
        out_shape=(grid_f32, grid_f32, grid_f32, jax.ShapeDtypeStruct((SUB, LANE), F32), pay2),
        in_specs=[smem] + [vmem] * 8,
        out_specs=(vmem,) * 5,
        scratch_shapes=scratch + [pltpu.VMEM((2 * tiles, LANE), F32)] + tail,
        compiler_params=pltpu.CompilerParams(vmem_limit_bytes=VMEM_LIMIT),
        name="middle",
    )(me, got, init_tile, keep, base, cum_a, cum_b, diag, recur_weight)
    got = exchange(pay)

    fresh, cum_a, one = pl.pallas_call(
        functools.partial(step_kernel, True),
        out_shape=(turned, turned, last1),
        in_specs=[smem] + [vmem] * 10,
        out_specs=(vmem,) * 3,
        scratch_shapes=scratch + tail,
        compiler_params=pltpu.CompilerParams(vmem_limit_bytes=VMEM_LIMIT),
        name="last",
    )(me, got, init_tile, keep, base, cum_a, cum_b, diag, recur_weight, state, moved)

    other = lax.ppermute(one, "tm", [(k, k ^ 1) for k in range(peers)])
    pay = pl.pallas_call(
        pair_kernel,
        out_shape=last8,
        in_specs=[smem] + [vmem] * 2,
        out_specs=vmem,
        scratch_shapes=[pltpu.VMEM(last1.shape, F32)],
        compiler_params=pltpu.CompilerParams(vmem_limit_bytes=VMEM_LIMIT),
        name="pair",
    )(me, one, other)
    got = exchange(pay, [[2 * k + s for k in range(peers // 2)] for s in range(2)])

    path, norms = pl.pallas_call(
        functools.partial(final_kernel, peers * rows * width),
        out_shape=(grid_f32, jax.ShapeDtypeStruct((3,), F32)),
        in_specs=[smem] + [vmem] * 4,
        out_specs=(hbm, hbm),
        scratch_shapes=[
            pltpu.VMEM((peers // 2, tiles, LANE), F32),
            pltpu.VMEM((tiles, LANE), F32),
            pltpu.VMEM((rows, width), F32),
            pltpu.SMEM((3,), F32),
            pltpu.SemaphoreType.DMA((CHUNKS + 1,)),
        ],
        compiler_params=pltpu.CompilerParams(vmem_limit_bytes=VMEM_LIMIT),
        name="final",
    )(me, got, other, fresh, cum_a)
    return path, norms


def solution(mesh):
    placed = (P("tm", "batch"), P("tm", "batch"), P("batch"), P("batch"), P())
    return jax.shard_map(
        body, mesh=mesh, in_specs=placed, out_specs=(P("tm", "batch"), P("batch")), check_vma=False
    )
```

```python
import functools

import jax
import jax.numpy as jnp
from jax import lax
from jax.experimental import pallas as pl
from jax.experimental.pallas import tpu as pltpu
from jax.sharding import PartitionSpec as P

SUB = 8
LANE = 128
WIDE = 256
PARTS = 2
CHUNKS = 2
ORDERS = {
    8: [4, 0, 7, 3, 1, 6, 5, 2],
    16: [11, 5, 13, 14, 10, 8, 6, 0, 3, 1, 4, 2, 7, 9, 15, 12],
}
VMEM_LIMIT = 16 * 1024 * 1024
F32 = jnp.float32
BF16 = jnp.bfloat16


LOG2E = 1.4426950408889634


def keep_of(gate, rate2):
    soft = jnp.maximum(gate, 0.0) + jnp.log(1.0 + jnp.exp2(jnp.abs(gate) * -LOG2E))
    return jnp.exp2(-rate2 * soft - jnp.maximum(gate * LOG2E - 8.0 * LOG2E, 0.0))


def chunk_scan(mul, add):
    run_a, run_b = [mul[0]], [add[0]]
    for a, b in zip(mul[1:], add[1:]):
        run_a.append(a * run_a[-1])
        run_b.append(a * run_b[-1] + b)
    tot_a, tot_b = run_a[-1], run_b[-1]
    place = lax.broadcasted_iota(jnp.int32, tot_a.shape, 0)
    shift = 1
    while shift < SUB:
        far = place >= shift
        old_a = jnp.where(far, pltpu.roll(tot_a, shift, 0), 1.0)
        old_b = jnp.where(far, pltpu.roll(tot_b, shift, 0), 0.0)
        tot_b = tot_a * old_b + tot_b
        tot_a = tot_a * old_a
        shift *= 2
    far = place >= 1
    head_a = jnp.where(far, pltpu.roll(tot_a, 1, 0), 1.0)
    head_b = jnp.where(far, pltpu.roll(tot_b, 1, 0), 0.0)
    cum_a = [a * head_a for a in run_a]
    cum_b = [a * head_b + b for a, b in zip(run_a, run_b)]
    return cum_a, cum_b


def write_rows(ref, base, first_tile, row):
    for k in range(row.shape[1] // LANE):
        ref[pl.ds(base + first_tile + k, 1), :] = row[:, k * LANE : (k + 1) * LANE]


def read_row(ref, first_tile, tiles):
    return jnp.concatenate([ref[pl.ds(first_tile + k, 1), :] for k in range(tiles)], axis=1)


def spread(one_ref, out_ref):
    value = one_ref[...]
    for q in range(out_ref.shape[0]):
        out_ref[q] = value


def start_kernel(
    me_ref, gate_hbm, cand_hbm, rates_hbm, init_hbm, w_hbm,
    keep_ref, base_ref, cum_a_ref, cum_b_ref, diag_ref, pay_ref,
    gate_ref, cand_ref, rates_ref, init_ref, w_ref, blocks, gate_nat, base_nat, mixed, one,
    in_sem, w_sem, d_sem,
):
    rows, width = gate_ref.shape
    steps = rows // SUB
    tiles = width // LANE
    per = WIDE // LANE
    part = width // PARTS
    me = me_ref[0]

    def columns(hbm, ref, k, sem):
        cols = pl.ds(k * part, part)
        return pltpu.make_async_copy(hbm.at[:, cols], ref.at[:, cols], sem)

    rates_copy = pltpu.make_async_copy(rates_hbm, rates_ref, in_sem.at[2 * PARTS])
    init_copy = pltpu.make_async_copy(init_hbm, init_ref, in_sem.at[2 * PARTS + 1])
    gate_copies = [columns(gate_hbm, gate_ref, k, in_sem.at[k]) for k in range(PARTS)]
    cand_copies = [columns(cand_hbm, cand_ref, k, in_sem.at[PARTS + k]) for k in range(PARTS)]
    diag_copies = [
        pltpu.make_async_copy(
            w_hbm.at[pl.ds(k * LANE, LANE), pl.ds(k * LANE, LANE)], blocks.at[k], d_sem.at[k]
        )
        for k in range(tiles)
    ]
    w_copies = [
        pltpu.make_async_copy(
            w_hbm.at[pl.ds(k * part, part), :], w_ref.at[pl.ds(k * part, part), :], w_sem.at[k]
        )
        for k in range(PARTS)
    ]
    for k in range(PARTS):
        gate_copies[k].start()
        cand_copies[k].start()
    rates_copy.start()
    init_copy.start()
    for copy in diag_copies:
        copy.start()

    @pl.when(me == 0)
    def _():
        for copy in w_copies:
            copy.start()

    mixed[...] = jnp.zeros_like(mixed)
    rates_copy.wait()
    init_copy.wait()
    for copy in diag_copies:
        copy.wait()

    @pl.when(me == 0)
    def _():
        total = jnp.zeros((SUB, width), F32)
        for k in range(PARTS):
            w_copies[k].wait()
            left = jnp.broadcast_to(init_ref[:, k * part : (k + 1) * part], (SUB, part)).astype(BF16)
            total = total + jnp.dot(left, w_ref[k * part : (k + 1) * part, :], preferred_element_type=F32)
        mixed[...] = total[0:1, :]

    @pl.when(me != 0)
    def _():
        init_ref[...] = jnp.zeros_like(init_ref)

    turn = [pl.ds(r, SUB, stride=steps) for r in range(steps)]
    for p in range(PARTS):
        gate_copies[p].wait()
        cand_copies[p].wait()

        @pl.loop(p * (part // WIDE), (p + 1) * (part // WIDE), unroll=True)
        def _(j):
            cols = pl.ds(pl.multiple_of(j * WIDE, WIDE), WIDE)
            on_diag = lax.broadcasted_iota(jnp.int32, (LANE, LANE), 0) == lax.broadcasted_iota(
                jnp.int32, (LANE, LANE), 1
            )
            units = []
            for k in range(per):
                here = pl.ds(pl.multiple_of(j * WIDE + k * LANE, LANE), LANE)
                gate_nat[j * per + k] = gate_ref[:, here].astype(F32)
                base_nat[j * per + k] = cand_ref[:, here].astype(F32)
                block = jnp.where(on_diag, blocks[j * per + k].astype(F32), 0.0)
                units.append(jnp.sum(block, axis=0, keepdims=True))
            unit = jnp.concatenate(units, axis=1)
            diag_ref[:, cols] = unit
            top = lax.broadcasted_iota(jnp.int32, (SUB, WIDE), 0) == 0
            rate = rates_ref[:, cols] * LOG2E
            mul, add = [], []
            for r in range(steps):
                here = pl.ds(r * SUB, SUB)
                gate = jnp.concatenate([gate_nat[j * per + k, turn[r], :] for k in range(per)], axis=1)
                base = jnp.concatenate([base_nat[j * per + k, turn[r], :] for k in range(per)], axis=1)
                keep = keep_of(gate, rate)
                keep_ref[here, cols] = keep
                base_ref[here, cols] = base
                left = 1.0 - keep
                cand = jnp.tanh(base + jnp.where(top, mixed[:, cols], 0.0) if r == 0 else base)
                slope = keep + left * (1.0 - cand * cand) * unit
                offset = left * cand
                if r == 0:
                    prev = jnp.where(top, init_ref[:, cols], 0.0)
                    offset = (keep * prev + offset) - slope * prev
                mul.append(slope)
                add.append(offset)
            cum_a, cum_b = chunk_scan(mul, add)
            for r in range(steps):
                here = pl.ds(r * SUB, SUB)
                cum_a_ref[here, cols] = cum_a[r]
                cum_b_ref[here, cols] = cum_b[r]
            write_rows(one, 0, j * per, cum_a[-1][SUB - 1 :, :])
            write_rows(one, tiles, j * per, cum_b[-1][SUB - 1 :, :])

    spread(one, pay_ref)


def step_kernel(
    last, me_ref, got_ref, init_ref, keep_ref, base_ref, cum_a_ref, cum_b_ref, diag_ref, w_ref, old_ref, tot_ref,
    *rest,
):
    if last:
        fresh_ref, out_a_ref, one, prev, low, entry, acc, mix = rest
    else:
        state_ref, out_a_ref, out_b_ref, sum_ref, pay_ref, prev, low, entry, one, acc, mix = rest
    rows, width = keep_ref.shape
    steps = rows // SUB
    tiles = width // LANE
    per = WIDE // LANE

    e = init_ref[...]
    order = order_of(got_ref.shape[0])
    for q in range(got_ref.shape[0] - 1):
        k = order.index(q)
        e = jnp.where(q < me_ref[0], got_ref[k, 0:tiles, :] * e + got_ref[k, tiles : 2 * tiles, :], e)
    entry[...] = e
    acc[...] = jnp.zeros_like(acc)

    def turned_state(j):
        cols = slice(j * WIDE, (j + 1) * WIDE)
        e = read_row(entry, j * per, per)
        state = [
            cum_b_ref[pl.ds(r * SUB, SUB), cols] + cum_a_ref[pl.ds(r * SUB, SUB), cols] * e for r in range(steps)
        ]
        place = lax.broadcasted_iota(jnp.int32, state[0].shape, 0)
        before = [jnp.where(place == 0, jnp.broadcast_to(e, state[0].shape), pltpu.roll(state[-1], 1, 0))] + state[:-1]
        moved = 0.0
        for r in range(steps):
            prev[pl.ds(r * SUB, SUB), cols] = before[r]
            change = state[r] if old_ref is None else state[r] - old_ref[pl.ds(r * SUB, SUB), cols]
            moved = moved + change * change
            if not last:
                state_ref[pl.ds(r * SUB, SUB), cols] = state[r]
        rounded = jnp.concatenate(before, axis=0).astype(BF16)
        low[:, cols] = rounded
        acc[...] += sum(moved[:, k * LANE : (k + 1) * LANE] for k in range(per))
        return jnp.dot(rounded, w_ref[cols, 0:WIDE], preferred_element_type=F32)

    mix[0] = sum(turned_state(j) for j in range(width // WIDE))
    if not last:
        sum_ref[...] = acc[...]
    else:
        one[pl.ds(4 * tiles, SUB), :] = jnp.zeros((SUB, LANE), F32)
        one[pl.ds(4 * tiles, 1), :] = jnp.sum(tot_ref[...], axis=0, keepdims=True)
        one[pl.ds(4 * tiles + 1, 1), :] = jnp.sum(acc[...], axis=0, keepdims=True)
        acc[...] = jnp.zeros_like(acc)

    def multiply(j, slot):
        cols = pl.ds(pl.multiple_of(j * WIDE, WIDE), WIDE)
        mix[slot] = jnp.dot(low[...], w_ref[:, cols], preferred_element_type=F32)

    def solve(j, slot):
        cols = pl.ds(pl.multiple_of(j * WIDE, WIDE), WIDE)
        unit = diag_ref[:, cols]
        mul, add = [], []
        for r in range(steps):
            here = pl.ds(r * SUB, SUB)
            keep = keep_ref[here, cols]
            before = prev[here, cols]
            cand = jnp.tanh(base_ref[here, cols] + mix[slot, here, :])
            left = 1.0 - keep
            mapped = keep * before + left * cand
            slope = keep + left * (1.0 - cand * cand) * unit
            mul.append(slope)
            add.append(mapped - slope * before)
        cum_a, cum_b = chunk_scan(mul, add)
        if last:
            e = read_row(entry, j * per, per)
            c0, c1, c2 = 0.0, 0.0, 0.0
            for r in range(steps):
                here = pl.ds(r * SUB, SUB)
                fresh = cum_b[r] + cum_a[r] * e
                if r + 1 < steps:
                    state = prev[pl.ds((r + 1) * SUB, SUB), cols]
                else:
                    state = cum_b_ref[here, cols] + cum_a_ref[here, cols] * e
                u = fresh - state
                for k in range(per):
                    part = slice(k * LANE, (k + 1) * LANE)
                    fresh_ref[j * per + k, pl.ds(r, SUB, stride=steps), :] = fresh[:, part]
                    out_a_ref[j * per + k, pl.ds(r, SUB, stride=steps), :] = cum_a[r][:, part]
                c0 = c0 + u * u
                c1 = c1 + u * cum_a[r]
                c2 = c2 + cum_a[r] * cum_a[r]
            acc[...] += sum(c0[:, k * LANE : (k + 1) * LANE] for k in range(per))
            write_rows(one, 0, j * per, cum_a[-1][SUB - 1 :, :])
            write_rows(one, tiles, j * per, u[SUB - 1 :, :])
            write_rows(one, 2 * tiles, j * per, 2.0 * jnp.sum(c1, axis=0, keepdims=True))
            write_rows(one, 3 * tiles, j * per, jnp.sum(c2, axis=0, keepdims=True))
        else:
            for r in range(steps):
                here = pl.ds(r * SUB, SUB)
                out_a_ref[here, cols] = cum_a[r]
                out_b_ref[here, cols] = cum_b[r]
            write_rows(one, 0, j * per, cum_a[-1][SUB - 1 :, :])
            write_rows(one, tiles, j * per, cum_b[-1][SUB - 1 :, :])

    blocks = width // WIDE

    @pl.loop(0, blocks // 2 - 1, unroll=True)
    def _(i):
        multiply(2 * i + 1, 1)
        solve(2 * i, 0)
        multiply(2 * i + 2, 0)
        solve(2 * i + 1, 1)

    multiply(blocks - 1, 1)
    solve(blocks - 2, 0)
    solve(blocks - 1, 1)
    if last:
        one[pl.ds(4 * tiles + 2, 1), :] = jnp.sum(acc[...], axis=0, keepdims=True)
    else:
        spread(one, pay_ref)


def first_step_kernel(me, got, init, keep, base, cum_a, cum_b, diag, w, *rest):
    step_kernel(False, me, got, init, keep, base, cum_a, cum_b, diag, w, None, None, *rest)


def pair_kernel(me_ref, one_ref, other_ref, pay_ref, both):
    tiles = (one_ref.shape[0] - SUB) // 4

    def join(first, second):
        a1, b1, l1, q1 = (first[k * tiles : (k + 1) * tiles, :] for k in range(4))
        a2, b2, l2, q2 = (second[k * tiles : (k + 1) * tiles, :] for k in range(4))
        both[0:tiles, :] = a1 * a2
        both[tiles : 2 * tiles, :] = a2 * b1 + b2
        both[2 * tiles : 3 * tiles, :] = l1 + a1 * (l2 + 2.0 * q2 * b1)
        both[3 * tiles : 4 * tiles, :] = q1 + a1 * a1 * q2
        both[4 * tiles :, :] = first[4 * tiles :, :] + second[4 * tiles :, :]
        extra = jnp.sum(b1 * (l2 + q2 * b1), axis=0, keepdims=True)
        both[4 * tiles + 2 : 4 * tiles + 3, :] = both[4 * tiles + 2 : 4 * tiles + 3, :] + extra

    @pl.when(lax.rem(me_ref[0], 2) == 0)
    def _():
        join(one_ref, other_ref)

    @pl.when(lax.rem(me_ref[0], 2) == 1)
    def _():
        join(other_ref, one_ref)

    spread(both, pay_ref)


def final_kernel(
    count, me_ref, got_ref, other_ref, fresh_ref, cum_a_ref, path_hbm, norm_hbm, moves, entry, path, norm_ref, sem
):
    tiles, rows, _ = fresh_ref.shape
    pairs = got_ref.shape[0]
    order = order_of(pairs)
    moves[0] = jnp.zeros((tiles, LANE), F32)
    d = moves[0]
    for q in range(pairs - 1):
        k = order.index(q)
        d = got_ref[k, 0:tiles, :] * d + got_ref[k, tiles : 2 * tiles, :]
        moves[q + 1] = d
    entry[...] = moves[lax.div(me_ref[0], 2)]

    @pl.when(lax.rem(me_ref[0], 2) == 1)
    def _():
        entry[...] = other_ref[0:tiles, :] * entry[...] + other_ref[tiles : 2 * tiles, :]

    copies = []
    for p in range(CHUNKS):
        for j in range(p * tiles // CHUNKS, (p + 1) * tiles // CHUNKS):
            path[:, j * LANE : (j + 1) * LANE] = fresh_ref[j] + cum_a_ref[j] * entry[j : j + 1, :]
        here = pl.ds(p * (tiles // CHUNKS) * LANE, (tiles // CHUNKS) * LANE)
        copies.append(pltpu.make_async_copy(path.at[:, here], path_hbm.at[:, here], sem.at[p]))
        copies[-1].start()

    quad, sums = moves[0], moves[0, 0:SUB, :]
    for q in range(pairs):
        k = order.index(q)
        d = moves[q]
        quad = quad + d * (got_ref[k, 2 * tiles : 3 * tiles, :] + got_ref[k, 3 * tiles : 4 * tiles, :] * d)
        sums = sums + got_ref[k, 4 * tiles : 4 * tiles + SUB, :]
    extra = jnp.sum(quad, axis=0, keepdims=True)
    totals = [sums[0:1, :], sums[1:2, :], sums[2:3, :] + extra]
    for k, row in enumerate(totals):
        total = jnp.sum(row, axis=1, keepdims=True)
        norm_ref[k] = jnp.max(jnp.sqrt(total / count))
    copies.append(pltpu.make_async_copy(norm_ref, norm_hbm, sem.at[CHUNKS]))
    copies[-1].start()
    for copy in copies:
        copy.wait()


def order_of(count):
    ends = [count - 1 - k // 2 if k % 2 == 0 else k // 2 for k in range(count)]
    return ORDERS.get(count, ends)


def exchange(pay, every):
    order = order_of(pay.shape[0])
    return lax.all_to_all(pay, "tm", 0, 0, axis_index_groups=[[every * k + s for k in order] for s in range(every)])


def body(gate_in, cand_in, rates, init_state, recur_weight):
    rows, width = gate_in.shape
    peers = lax.axis_size("tm")
    tiles = width // LANE
    steps = rows // SUB
    assert rows % (2 * SUB) == 0 and width % (2 * WIDE) == 0 and peers % 2 == 0
    me = lax.axis_index("tm").astype(jnp.int32).reshape(1)
    init_row = init_state.reshape(1, width)
    init_tile = init_state.reshape(tiles, LANE)
    vmem = pl.BlockSpec(memory_space=pltpu.VMEM)
    smem = pl.BlockSpec(memory_space=pltpu.SMEM)
    hbm = pl.BlockSpec(memory_space=pltpu.HBM)
    grid_f32 = jax.ShapeDtypeStruct((rows, width), F32)
    pay2 = jax.ShapeDtypeStruct((peers, 2 * tiles, LANE), F32)
    last1 = jax.ShapeDtypeStruct((4 * tiles + SUB, LANE), F32)
    last8 = jax.ShapeDtypeStruct((peers // 2, 4 * tiles + SUB, LANE), F32)
    turned = jax.ShapeDtypeStruct((tiles, rows, LANE), F32)

    keep, base, cum_a, cum_b, diag, pay = pl.pallas_call(
        start_kernel,
        out_shape=(grid_f32, grid_f32, grid_f32, grid_f32, jax.ShapeDtypeStruct((1, width), F32), pay2),
        in_specs=[smem] + [hbm] * 5,
        out_specs=(vmem,) * 6,
        scratch_shapes=[
            pltpu.VMEM((rows, width), BF16),
            pltpu.VMEM((rows, width), BF16),
            pltpu.VMEM((1, width), F32),
            pltpu.VMEM((1, width), F32),
            pltpu.VMEM((width, width), BF16),
            pltpu.VMEM((tiles, LANE, LANE), BF16),
            pltpu.VMEM((tiles, rows, LANE), F32),
            pltpu.VMEM((tiles, rows, LANE), F32),
            pltpu.VMEM((1, width), F32),
            pltpu.VMEM((2 * tiles, LANE), F32),
            pltpu.SemaphoreType.DMA((2 * PARTS + 2,)),
            pltpu.SemaphoreType.DMA((PARTS,)),
            pltpu.SemaphoreType.DMA((tiles,)),
        ],
        compiler_params=pltpu.CompilerParams(vmem_limit_bytes=VMEM_LIMIT),
        name="start",
    )(me, *(pltpu.with_memory_space_constraint(x, pltpu.HBM) for x in (gate_in, cand_in, rates.reshape(1, width), init_row, recur_weight)))
    got = exchange(pay, 1)

    scratch = [
        pltpu.VMEM((rows, width), F32),
        pltpu.VMEM((rows, width), BF16),
        pltpu.VMEM((tiles, LANE), F32),
    ]
    tail = [pltpu.VMEM((SUB, LANE), F32), pltpu.VMEM((2, rows, WIDE), F32)]
    state, cum_a, cum_b, moved, pay = pl.pallas_call(
        first_step_kernel,
        out_shape=(grid_f32, grid_f32, grid_f32, jax.ShapeDtypeStruct((SUB, LANE), F32), pay2),
        in_specs=[smem] + [vmem] * 8,
        out_specs=(vmem,) * 5,
        scratch_shapes=scratch + [pltpu.VMEM((2 * tiles, LANE), F32)] + tail,
        compiler_params=pltpu.CompilerParams(vmem_limit_bytes=VMEM_LIMIT),
        name="middle",
    )(me, got, init_tile, keep, base, cum_a, cum_b, diag, recur_weight)
    got = exchange(pay, 1)

    fresh, cum_a, one = pl.pallas_call(
        functools.partial(step_kernel, True),
        out_shape=(turned, turned, last1),
        in_specs=[smem] + [vmem] * 10,
        out_specs=(vmem,) * 3,
        scratch_shapes=scratch + tail,
        compiler_params=pltpu.CompilerParams(vmem_limit_bytes=VMEM_LIMIT),
        name="last",
    )(me, got, init_tile, keep, base, cum_a, cum_b, diag, recur_weight, state, moved)

    other = lax.ppermute(one, "tm", [(k, k ^ 1) for k in range(peers)])
    pay = pl.pallas_call(
        pair_kernel,
        out_shape=last8,
        in_specs=[smem] + [vmem] * 2,
        out_specs=vmem,
        scratch_shapes=[pltpu.VMEM(last1.shape, F32)],
        compiler_params=pltpu.CompilerParams(vmem_limit_bytes=VMEM_LIMIT),
        name="pair",
    )(me, one, other)
    got = exchange(pay, 2)

    path, norms = pl.pallas_call(
        functools.partial(final_kernel, peers * rows * width),
        out_shape=(grid_f32, jax.ShapeDtypeStruct((3,), F32)),
        in_specs=[smem] + [vmem] * 4,
        out_specs=(hbm, hbm),
        scratch_shapes=[
            pltpu.VMEM((peers // 2, tiles, LANE), F32),
            pltpu.VMEM((tiles, LANE), F32),
            pltpu.VMEM((rows, width), F32),
            pltpu.SMEM((3,), F32),
            pltpu.SemaphoreType.DMA((CHUNKS + 1,)),
        ],
        compiler_params=pltpu.CompilerParams(vmem_limit_bytes=VMEM_LIMIT),
        name="final",
    )(me, got, other, fresh, cum_a)
    return path, norms


def solution(mesh):
    placed = (P("tm", "batch"), P("tm", "batch"), P("batch"), P("batch"), P())
    return jax.shard_map(
        body, mesh=mesh, in_specs=placed, out_specs=(P("tm", "batch"), P("batch")), check_vma=False
    )
```

```python
import functools

import jax
import jax.numpy as jnp
from jax import lax
from jax.experimental import pallas as pl
from jax.experimental.pallas import tpu as pltpu
from jax.sharding import PartitionSpec as P

SUB = 8
LANE = 128
WIDE = 256
PARTS = 2
CHUNKS = 2
ORDERS = {
    (16, 0): [5, 14, 10, 8, 13, 0, 3, 1, 4, 11, 2, 7, 6, 9, 15, 12],
    (16, 1): [9, 5, 13, 14, 10, 8, 6, 15, 2, 1, 4, 3, 7, 11, 0, 12],
    (8, 2): [4, 0, 7, 3, 1, 6, 5, 2],
}
VMEM_LIMIT = 16 * 1024 * 1024
F32 = jnp.float32
BF16 = jnp.bfloat16


LOG2E = 1.4426950408889634


def keep_of(gate, rate2):
    soft = jnp.maximum(gate, 0.0) + jnp.log(1.0 + jnp.exp2(jnp.abs(gate) * -LOG2E))
    return jnp.exp2(-rate2 * soft - jnp.maximum(gate * LOG2E - 8.0 * LOG2E, 0.0))


def chunk_scan(mul, add):
    run_a, run_b = [mul[0]], [add[0]]
    for a, b in zip(mul[1:], add[1:]):
        run_a.append(a * run_a[-1])
        run_b.append(a * run_b[-1] + b)
    tot_a, tot_b = run_a[-1], run_b[-1]
    place = lax.broadcasted_iota(jnp.int32, tot_a.shape, 0)
    shift = 1
    while shift < SUB:
        far = place >= shift
        old_a = jnp.where(far, pltpu.roll(tot_a, shift, 0), 1.0)
        old_b = jnp.where(far, pltpu.roll(tot_b, shift, 0), 0.0)
        tot_b = tot_a * old_b + tot_b
        tot_a = tot_a * old_a
        shift *= 2
    far = place >= 1
    head_a = jnp.where(far, pltpu.roll(tot_a, 1, 0), 1.0)
    head_b = jnp.where(far, pltpu.roll(tot_b, 1, 0), 0.0)
    cum_a = [a * head_a for a in run_a]
    cum_b = [a * head_b + b for a, b in zip(run_a, run_b)]
    return cum_a, cum_b


def write_rows(ref, base, first_tile, row):
    for k in range(row.shape[1] // LANE):
        ref[pl.ds(base + first_tile + k, 1), :] = row[:, k * LANE : (k + 1) * LANE]


def read_row(ref, first_tile, tiles):
    return jnp.concatenate([ref[pl.ds(first_tile + k, 1), :] for k in range(tiles)], axis=1)


def spread(one_ref, out_ref):
    value = one_ref[...]
    for q in range(out_ref.shape[0]):
        out_ref[q] = value


def start_kernel(
    me_ref, gate_hbm, cand_hbm, rates_hbm, init_hbm, w_hbm,
    keep_ref, base_ref, cum_a_ref, cum_b_ref, diag_ref, pay_ref,
    gate_ref, cand_ref, rates_ref, init_ref, w_ref, blocks, gate_nat, base_nat, mixed, one,
    in_sem, w_sem, d_sem,
):
    rows, width = gate_ref.shape
    steps = rows // SUB
    tiles = width // LANE
    per = WIDE // LANE
    part = width // PARTS
    me = me_ref[0]

    def columns(hbm, ref, k, sem):
        cols = pl.ds(k * part, part)
        return pltpu.make_async_copy(hbm.at[:, cols], ref.at[:, cols], sem)

    rates_copy = pltpu.make_async_copy(rates_hbm, rates_ref, in_sem.at[2 * PARTS])
    init_copy = pltpu.make_async_copy(init_hbm, init_ref, in_sem.at[2 * PARTS + 1])
    gate_copies = [columns(gate_hbm, gate_ref, k, in_sem.at[k]) for k in range(PARTS)]
    cand_copies = [columns(cand_hbm, cand_ref, k, in_sem.at[PARTS + k]) for k in range(PARTS)]
    diag_copies = [
        pltpu.make_async_copy(
            w_hbm.at[pl.ds(k * LANE, LANE), pl.ds(k * LANE, LANE)], blocks.at[k], d_sem.at[k]
        )
        for k in range(tiles)
    ]
    w_copies = [
        pltpu.make_async_copy(
            w_hbm.at[pl.ds(k * part, part), :], w_ref.at[pl.ds(k * part, part), :], w_sem.at[k]
        )
        for k in range(PARTS)
    ]
    for k in range(PARTS):
        gate_copies[k].start()
        cand_copies[k].start()
    rates_copy.start()
    init_copy.start()
    for copy in diag_copies:
        copy.start()

    @pl.when(me == 0)
    def _():
        for copy in w_copies:
            copy.start()

    mixed[...] = jnp.zeros_like(mixed)
    rates_copy.wait()
    init_copy.wait()
    for copy in diag_copies:
        copy.wait()

    @pl.when(me == 0)
    def _():
        total = jnp.zeros((SUB, width), F32)
        for k in range(PARTS):
            w_copies[k].wait()
            left = jnp.broadcast_to(init_ref[:, k * part : (k + 1) * part], (SUB, part)).astype(BF16)
            total = total + jnp.dot(left, w_ref[k * part : (k + 1) * part, :], preferred_element_type=F32)
        mixed[...] = total[0:1, :]

    @pl.when(me != 0)
    def _():
        init_ref[...] = jnp.zeros_like(init_ref)

    turn = [pl.ds(r, SUB, stride=steps) for r in range(steps)]
    for p in range(PARTS):
        gate_copies[p].wait()
        cand_copies[p].wait()

        @pl.loop(p * (part // WIDE), (p + 1) * (part // WIDE), unroll=True)
        def _(j):
            cols = pl.ds(pl.multiple_of(j * WIDE, WIDE), WIDE)
            on_diag = lax.broadcasted_iota(jnp.int32, (LANE, LANE), 0) == lax.broadcasted_iota(
                jnp.int32, (LANE, LANE), 1
            )
            units = []
            for k in range(per):
                here = pl.ds(pl.multiple_of(j * WIDE + k * LANE, LANE), LANE)
                gate_nat[j * per + k] = gate_ref[:, here].astype(F32)
                base_nat[j * per + k] = cand_ref[:, here].astype(F32)
                block = jnp.where(on_diag, blocks[j * per + k].astype(F32), 0.0)
                units.append(jnp.sum(block, axis=0, keepdims=True))
            unit = jnp.concatenate(units, axis=1)
            diag_ref[:, cols] = unit
            top = lax.broadcasted_iota(jnp.int32, (SUB, WIDE), 0) == 0
            rate = rates_ref[:, cols] * LOG2E
            mul, add = [], []
            for r in range(steps):
                here = pl.ds(r * SUB, SUB)
                gate = jnp.concatenate([gate_nat[j * per + k, turn[r], :] for k in range(per)], axis=1)
                base = jnp.concatenate([base_nat[j * per + k, turn[r], :] for k in range(per)], axis=1)
                keep = keep_of(gate, rate)
                keep_ref[here, cols] = keep
                base_ref[here, cols] = base
                left = 1.0 - keep
                cand = jnp.tanh(base + jnp.where(top, mixed[:, cols], 0.0) if r == 0 else base)
                slope = keep + left * (1.0 - cand * cand) * unit
                offset = left * cand
                if r == 0:
                    prev = jnp.where(top, init_ref[:, cols], 0.0)
                    offset = (keep * prev + offset) - slope * prev
                mul.append(slope)
                add.append(offset)
            cum_a, cum_b = chunk_scan(mul, add)
            for r in range(steps):
                here = pl.ds(r * SUB, SUB)
                cum_a_ref[here, cols] = cum_a[r]
                cum_b_ref[here, cols] = cum_b[r]
            write_rows(one, 0, j * per, cum_a[-1][SUB - 1 :, :])
            write_rows(one, tiles, j * per, cum_b[-1][SUB - 1 :, :])

    spread(one, pay_ref)


def step_kernel(
    last, me_ref, got_ref, init_ref, keep_ref, base_ref, cum_a_ref, cum_b_ref, diag_ref, w_ref, old_ref, tot_ref,
    *rest,
):
    if last:
        fresh_ref, out_a_ref, one, prev, low, entry, acc, mix = rest
    else:
        state_ref, out_a_ref, out_b_ref, sum_ref, pay_ref, prev, low, entry, one, acc, mix = rest
    rows, width = keep_ref.shape
    steps = rows // SUB
    tiles = width // LANE
    per = WIDE // LANE

    e = init_ref[...]
    order = order_of(got_ref.shape[0], int(last))
    for q in range(got_ref.shape[0] - 1):
        k = order.index(q)
        e = jnp.where(q < me_ref[0], got_ref[k, 0:tiles, :] * e + got_ref[k, tiles : 2 * tiles, :], e)
    entry[...] = e
    acc[...] = jnp.zeros_like(acc)

    def turned_state(j):
        cols = slice(j * WIDE, (j + 1) * WIDE)
        e = read_row(entry, j * per, per)
        state = [
            cum_b_ref[pl.ds(r * SUB, SUB), cols] + cum_a_ref[pl.ds(r * SUB, SUB), cols] * e for r in range(steps)
        ]
        place = lax.broadcasted_iota(jnp.int32, state[0].shape, 0)
        before = [jnp.where(place == 0, jnp.broadcast_to(e, state[0].shape), pltpu.roll(state[-1], 1, 0))] + state[:-1]
        moved = 0.0
        for r in range(steps):
            prev[pl.ds(r * SUB, SUB), cols] = before[r]
            change = state[r] if old_ref is None else state[r] - old_ref[pl.ds(r * SUB, SUB), cols]
            moved = moved + change * change
            if not last:
                state_ref[pl.ds(r * SUB, SUB), cols] = state[r]
        rounded = jnp.concatenate(before, axis=0).astype(BF16)
        low[:, cols] = rounded
        acc[...] += sum(moved[:, k * LANE : (k + 1) * LANE] for k in range(per))
        return jnp.dot(rounded, w_ref[cols, 0:WIDE], preferred_element_type=F32)

    mix[0] = sum(turned_state(j) for j in range(width // WIDE))
    if not last:
        sum_ref[...] = acc[...]
    else:
        one[pl.ds(4 * tiles, SUB), :] = jnp.zeros((SUB, LANE), F32)
        one[pl.ds(4 * tiles, 1), :] = jnp.sum(tot_ref[...], axis=0, keepdims=True)
        one[pl.ds(4 * tiles + 1, 1), :] = jnp.sum(acc[...], axis=0, keepdims=True)
        acc[...] = jnp.zeros_like(acc)

    def multiply(j, slot):
        cols = pl.ds(pl.multiple_of(j * WIDE, WIDE), WIDE)
        mix[slot] = jnp.dot(low[...], w_ref[:, cols], preferred_element_type=F32)

    def solve(j, slot):
        cols = pl.ds(pl.multiple_of(j * WIDE, WIDE), WIDE)
        unit = diag_ref[:, cols]
        mul, add = [], []
        for r in range(steps):
            here = pl.ds(r * SUB, SUB)
            keep = keep_ref[here, cols]
            before = prev[here, cols]
            cand = jnp.tanh(base_ref[here, cols] + mix[slot, here, :])
            left = 1.0 - keep
            mapped = keep * before + left * cand
            slope = keep + left * (1.0 - cand * cand) * unit
            mul.append(slope)
            add.append(mapped - slope * before)
        cum_a, cum_b = chunk_scan(mul, add)
        if last:
            e = read_row(entry, j * per, per)
            c0, c1, c2 = 0.0, 0.0, 0.0
            for r in range(steps):
                here = pl.ds(r * SUB, SUB)
                fresh = cum_b[r] + cum_a[r] * e
                if r + 1 < steps:
                    state = prev[pl.ds((r + 1) * SUB, SUB), cols]
                else:
                    state = cum_b_ref[here, cols] + cum_a_ref[here, cols] * e
                u = fresh - state
                for k in range(per):
                    part = slice(k * LANE, (k + 1) * LANE)
                    fresh_ref[j * per + k, pl.ds(r, SUB, stride=steps), :] = fresh[:, part]
                    out_a_ref[j * per + k, pl.ds(r, SUB, stride=steps), :] = cum_a[r][:, part]
                c0 = c0 + u * u
                c1 = c1 + u * cum_a[r]
                c2 = c2 + cum_a[r] * cum_a[r]
            acc[...] += sum(c0[:, k * LANE : (k + 1) * LANE] for k in range(per))
            write_rows(one, 0, j * per, cum_a[-1][SUB - 1 :, :])
            write_rows(one, tiles, j * per, u[SUB - 1 :, :])
            write_rows(one, 2 * tiles, j * per, 2.0 * jnp.sum(c1, axis=0, keepdims=True))
            write_rows(one, 3 * tiles, j * per, jnp.sum(c2, axis=0, keepdims=True))
        else:
            for r in range(steps):
                here = pl.ds(r * SUB, SUB)
                out_a_ref[here, cols] = cum_a[r]
                out_b_ref[here, cols] = cum_b[r]
            write_rows(one, 0, j * per, cum_a[-1][SUB - 1 :, :])
            write_rows(one, tiles, j * per, cum_b[-1][SUB - 1 :, :])

    blocks = width // WIDE

    @pl.loop(0, blocks // 2 - 1, unroll=True)
    def _(i):
        multiply(2 * i + 1, 1)
        solve(2 * i, 0)
        multiply(2 * i + 2, 0)
        solve(2 * i + 1, 1)

    multiply(blocks - 1, 1)
    solve(blocks - 2, 0)
    solve(blocks - 1, 1)
    if last:
        one[pl.ds(4 * tiles + 2, 1), :] = jnp.sum(acc[...], axis=0, keepdims=True)
    else:
        spread(one, pay_ref)


def first_step_kernel(me, got, init, keep, base, cum_a, cum_b, diag, w, *rest):
    step_kernel(False, me, got, init, keep, base, cum_a, cum_b, diag, w, None, None, *rest)


def pair_kernel(me_ref, one_ref, other_ref, pay_ref, both):
    tiles = (one_ref.shape[0] - SUB) // 4

    def join(first, second):
        a1, b1, l1, q1 = (first[k * tiles : (k + 1) * tiles, :] for k in range(4))
        a2, b2, l2, q2 = (second[k * tiles : (k + 1) * tiles, :] for k in range(4))
        both[0:tiles, :] = a1 * a2
        both[tiles : 2 * tiles, :] = a2 * b1 + b2
        both[2 * tiles : 3 * tiles, :] = l1 + a1 * (l2 + 2.0 * q2 * b1)
        both[3 * tiles : 4 * tiles, :] = q1 + a1 * a1 * q2
        both[4 * tiles :, :] = first[4 * tiles :, :] + second[4 * tiles :, :]
        extra = jnp.sum(b1 * (l2 + q2 * b1), axis=0, keepdims=True)
        both[4 * tiles + 2 : 4 * tiles + 3, :] = both[4 * tiles + 2 : 4 * tiles + 3, :] + extra

    @pl.when(lax.rem(me_ref[0], 2) == 0)
    def _():
        join(one_ref, other_ref)

    @pl.when(lax.rem(me_ref[0], 2) == 1)
    def _():
        join(other_ref, one_ref)

    spread(both, pay_ref)


def final_kernel(
    count, me_ref, got_ref, other_ref, fresh_ref, cum_a_ref, path_hbm, norm_hbm, moves, entry, path, norm_ref, sem
):
    tiles, rows, _ = fresh_ref.shape
    pairs = got_ref.shape[0]
    order = order_of(pairs, 2)
    moves[0] = jnp.zeros((tiles, LANE), F32)
    d = moves[0]
    for q in range(pairs - 1):
        k = order.index(q)
        d = got_ref[k, 0:tiles, :] * d + got_ref[k, tiles : 2 * tiles, :]
        moves[q + 1] = d
    entry[...] = moves[lax.div(me_ref[0], 2)]

    @pl.when(lax.rem(me_ref[0], 2) == 1)
    def _():
        entry[...] = other_ref[0:tiles, :] * entry[...] + other_ref[tiles : 2 * tiles, :]

    copies = []
    for p in range(CHUNKS):
        for j in range(p * tiles // CHUNKS, (p + 1) * tiles // CHUNKS):
            path[:, j * LANE : (j + 1) * LANE] = fresh_ref[j] + cum_a_ref[j] * entry[j : j + 1, :]
        here = pl.ds(p * (tiles // CHUNKS) * LANE, (tiles // CHUNKS) * LANE)
        copies.append(pltpu.make_async_copy(path.at[:, here], path_hbm.at[:, here], sem.at[p]))
        copies[-1].start()

    quad, sums = moves[0], moves[0, 0:SUB, :]
    for q in range(pairs):
        k = order.index(q)
        d = moves[q]
        quad = quad + d * (got_ref[k, 2 * tiles : 3 * tiles, :] + got_ref[k, 3 * tiles : 4 * tiles, :] * d)
        sums = sums + got_ref[k, 4 * tiles : 4 * tiles + SUB, :]
    extra = jnp.sum(quad, axis=0, keepdims=True)
    totals = [sums[0:1, :], sums[1:2, :], sums[2:3, :] + extra]
    for k, row in enumerate(totals):
        total = jnp.sum(row, axis=1, keepdims=True)
        norm_ref[k] = jnp.max(jnp.sqrt(total / count))
    copies.append(pltpu.make_async_copy(norm_ref, norm_hbm, sem.at[CHUNKS]))
    copies[-1].start()
    for copy in copies:
        copy.wait()


def order_of(count, stage):
    ends = [count - 1 - k // 2 if k % 2 == 0 else k // 2 for k in range(count)]
    return ORDERS.get((count, stage), ends)


def exchange(pay, stage, every=1):
    order = order_of(pay.shape[0], stage)
    return lax.all_to_all(pay, "tm", 0, 0, axis_index_groups=[[every * k + s for k in order] for s in range(every)])


def body(gate_in, cand_in, rates, init_state, recur_weight):
    rows, width = gate_in.shape
    peers = lax.axis_size("tm")
    tiles = width // LANE
    steps = rows // SUB
    assert rows % (2 * SUB) == 0 and width % (2 * WIDE) == 0 and peers % 2 == 0
    me = lax.axis_index("tm").astype(jnp.int32).reshape(1)
    init_row = init_state.reshape(1, width)
    init_tile = init_state.reshape(tiles, LANE)
    vmem = pl.BlockSpec(memory_space=pltpu.VMEM)
    smem = pl.BlockSpec(memory_space=pltpu.SMEM)
    hbm = pl.BlockSpec(memory_space=pltpu.HBM)
    grid_f32 = jax.ShapeDtypeStruct((rows, width), F32)
    pay2 = jax.ShapeDtypeStruct((peers, 2 * tiles, LANE), F32)
    last1 = jax.ShapeDtypeStruct((4 * tiles + SUB, LANE), F32)
    last8 = jax.ShapeDtypeStruct((peers // 2, 4 * tiles + SUB, LANE), F32)
    turned = jax.ShapeDtypeStruct((tiles, rows, LANE), F32)

    keep, base, cum_a, cum_b, diag, pay = pl.pallas_call(
        start_kernel,
        out_shape=(grid_f32, grid_f32, grid_f32, grid_f32, jax.ShapeDtypeStruct((1, width), F32), pay2),
        in_specs=[smem] + [hbm] * 5,
        out_specs=(vmem,) * 6,
        scratch_shapes=[
            pltpu.VMEM((rows, width), BF16),
            pltpu.VMEM((rows, width), BF16),
            pltpu.VMEM((1, width), F32),
            pltpu.VMEM((1, width), F32),
            pltpu.VMEM((width, width), BF16),
            pltpu.VMEM((tiles, LANE, LANE), BF16),
            pltpu.VMEM((tiles, rows, LANE), F32),
            pltpu.VMEM((tiles, rows, LANE), F32),
            pltpu.VMEM((1, width), F32),
            pltpu.VMEM((2 * tiles, LANE), F32),
            pltpu.SemaphoreType.DMA((2 * PARTS + 2,)),
            pltpu.SemaphoreType.DMA((PARTS,)),
            pltpu.SemaphoreType.DMA((tiles,)),
        ],
        compiler_params=pltpu.CompilerParams(vmem_limit_bytes=VMEM_LIMIT),
        name="start",
    )(me, *(pltpu.with_memory_space_constraint(x, pltpu.HBM) for x in (gate_in, cand_in, rates.reshape(1, width), init_row, recur_weight)))
    got = exchange(pay, 0)

    scratch = [
        pltpu.VMEM((rows, width), F32),
        pltpu.VMEM((rows, width), BF16),
        pltpu.VMEM((tiles, LANE), F32),
    ]
    tail = [pltpu.VMEM((SUB, LANE), F32), pltpu.VMEM((2, rows, WIDE), F32)]
    state, cum_a, cum_b, moved, pay = pl.pallas_call(
        first_step_kernel,
        out_shape=(grid_f32, grid_f32, grid_f32, jax.ShapeDtypeStruct((SUB, LANE), F32), pay2),
        in_specs=[smem] + [vmem] * 8,
        out_specs=(vmem,) * 5,
        scratch_shapes=scratch + [pltpu.VMEM((2 * tiles, LANE), F32)] + tail,
        compiler_params=pltpu.CompilerParams(vmem_limit_bytes=VMEM_LIMIT),
        name="middle",
    )(me, got, init_tile, keep, base, cum_a, cum_b, diag, recur_weight)
    got = exchange(pay, 1)

    fresh, cum_a, one = pl.pallas_call(
        functools.partial(step_kernel, True),
        out_shape=(turned, turned, last1),
        in_specs=[smem] + [vmem] * 10,
        out_specs=(vmem,) * 3,
        scratch_shapes=scratch + tail,
        compiler_params=pltpu.CompilerParams(vmem_limit_bytes=VMEM_LIMIT),
        name="last",
    )(me, got, init_tile, keep, base, cum_a, cum_b, diag, recur_weight, state, moved)

    other = lax.ppermute(one, "tm", [(k, k ^ 1) for k in range(peers)])
    pay = pl.pallas_call(
        pair_kernel,
        out_shape=last8,
        in_specs=[smem] + [vmem] * 2,
        out_specs=vmem,
        scratch_shapes=[pltpu.VMEM(last1.shape, F32)],
        compiler_params=pltpu.CompilerParams(vmem_limit_bytes=VMEM_LIMIT),
        name="pair",
    )(me, one, other)
    got = exchange(pay, 2, every=2)

    path, norms = pl.pallas_call(
        functools.partial(final_kernel, peers * rows * width),
        out_shape=(grid_f32, jax.ShapeDtypeStruct((3,), F32)),
        in_specs=[smem] + [vmem] * 4,
        out_specs=(hbm, hbm),
        scratch_shapes=[
            pltpu.VMEM((peers // 2, tiles, LANE), F32),
            pltpu.VMEM((tiles, LANE), F32),
            pltpu.VMEM((rows, width), F32),
            pltpu.SMEM((3,), F32),
            pltpu.SemaphoreType.DMA((CHUNKS + 1,)),
        ],
        compiler_params=pltpu.CompilerParams(vmem_limit_bytes=VMEM_LIMIT),
        name="final",
    )(me, got, other, fresh, cum_a)
    return path, norms


def solution(mesh):
    placed = (P("tm", "batch"), P("tm", "batch"), P("batch"), P("batch"), P())
    return jax.shard_map(
        body, mesh=mesh, in_specs=placed, out_specs=(P("tm", "batch"), P("batch")), check_vma=False
    )
```

```python
import functools

import jax
import jax.numpy as jnp
from jax import lax
from jax.experimental import pallas as pl
from jax.experimental.pallas import tpu as pltpu
from jax.sharding import PartitionSpec as P

SUB = 8
LANE = 128
WIDE = 256
PARTS = 2
CHUNKS = 2
ORDERS = {
    (16, 0): [5, 7, 10, 8, 13, 0, 1, 4, 11, 2, 9, 6, 3, 14, 15, 12],
    (16, 1): [9, 5, 13, 14, 10, 8, 6, 15, 2, 1, 4, 3, 7, 11, 0, 12],
    (8, 2): [4, 0, 7, 3, 1, 6, 5, 2],
}
VMEM_LIMIT = 16 * 1024 * 1024
F32 = jnp.float32
BF16 = jnp.bfloat16


LOG2E = 1.4426950408889634


def keep_of(gate, rate2):
    soft = jnp.maximum(gate, 0.0) + jnp.log(1.0 + jnp.exp2(jnp.abs(gate) * -LOG2E))
    return jnp.exp2(-rate2 * soft - jnp.maximum(gate * LOG2E - 8.0 * LOG2E, 0.0))


def chunk_scan(mul, add):
    run_a, run_b = [mul[0]], [add[0]]
    for a, b in zip(mul[1:], add[1:]):
        run_a.append(a * run_a[-1])
        run_b.append(a * run_b[-1] + b)
    tot_a, tot_b = run_a[-1], run_b[-1]
    place = lax.broadcasted_iota(jnp.int32, tot_a.shape, 0)
    shift = 1
    while shift < SUB:
        far = place >= shift
        old_a = jnp.where(far, pltpu.roll(tot_a, shift, 0), 1.0)
        old_b = jnp.where(far, pltpu.roll(tot_b, shift, 0), 0.0)
        tot_b = tot_a * old_b + tot_b
        tot_a = tot_a * old_a
        shift *= 2
    far = place >= 1
    head_a = jnp.where(far, pltpu.roll(tot_a, 1, 0), 1.0)
    head_b = jnp.where(far, pltpu.roll(tot_b, 1, 0), 0.0)
    cum_a = [a * head_a for a in run_a]
    cum_b = [a * head_b + b for a, b in zip(run_a, run_b)]
    return cum_a, cum_b


def write_rows(ref, base, first_tile, row):
    for k in range(row.shape[1] // LANE):
        ref[pl.ds(base + first_tile + k, 1), :] = row[:, k * LANE : (k + 1) * LANE]


def read_row(ref, first_tile, tiles):
    return jnp.concatenate([ref[pl.ds(first_tile + k, 1), :] for k in range(tiles)], axis=1)


def spread(one_ref, out_ref):
    value = one_ref[...]
    for q in range(out_ref.shape[0]):
        out_ref[q] = value


def start_kernel(
    me_ref, gate_hbm, cand_hbm, rates_hbm, init_hbm, w_hbm,
    keep_ref, base_ref, cum_a_ref, cum_b_ref, diag_ref, pay_ref,
    gate_ref, cand_ref, rates_ref, init_ref, w_ref, blocks, gate_nat, base_nat, mixed, one,
    in_sem, w_sem, d_sem,
):
    rows, width = gate_ref.shape
    steps = rows // SUB
    tiles = width // LANE
    per = WIDE // LANE
    part = width // PARTS
    me = me_ref[0]

    def columns(hbm, ref, k, sem):
        cols = pl.ds(k * part, part)
        return pltpu.make_async_copy(hbm.at[:, cols], ref.at[:, cols], sem)

    rates_copy = pltpu.make_async_copy(rates_hbm, rates_ref, in_sem.at[2 * PARTS])
    init_copy = pltpu.make_async_copy(init_hbm, init_ref, in_sem.at[2 * PARTS + 1])
    gate_copies = [columns(gate_hbm, gate_ref, k, in_sem.at[k]) for k in range(PARTS)]
    cand_copies = [columns(cand_hbm, cand_ref, k, in_sem.at[PARTS + k]) for k in range(PARTS)]
    diag_copies = [
        pltpu.make_async_copy(
            w_hbm.at[pl.ds(k * LANE, LANE), pl.ds(k * LANE, LANE)], blocks.at[k], d_sem.at[k]
        )
        for k in range(tiles)
    ]
    w_copies = [
        pltpu.make_async_copy(
            w_hbm.at[pl.ds(k * part, part), :], w_ref.at[pl.ds(k * part, part), :], w_sem.at[k]
        )
        for k in range(PARTS)
    ]
    for k in range(PARTS):
        gate_copies[k].start()
        cand_copies[k].start()
    rates_copy.start()
    init_copy.start()
    for copy in diag_copies:
        copy.start()

    @pl.when(me == 0)
    def _():
        for copy in w_copies:
            copy.start()

    mixed[...] = jnp.zeros_like(mixed)
    rates_copy.wait()
    init_copy.wait()

    @pl.when(me == 0)
    def _():
        total = jnp.zeros((SUB, width), F32)
        for k in range(PARTS):
            w_copies[k].wait()
            left = jnp.broadcast_to(init_ref[:, k * part : (k + 1) * part], (SUB, part)).astype(BF16)
            total = total + jnp.dot(left, w_ref[k * part : (k + 1) * part, :], preferred_element_type=F32)
        mixed[...] = total[0:1, :]

    @pl.when(me != 0)
    def _():
        init_ref[...] = jnp.zeros_like(init_ref)

    turn = [pl.ds(r, SUB, stride=steps) for r in range(steps)]
    for p in range(PARTS):
        gate_copies[p].wait()
        cand_copies[p].wait()
        for copy in diag_copies[p * tiles // PARTS : (p + 1) * tiles // PARTS]:
            copy.wait()

        @pl.loop(p * (part // WIDE), (p + 1) * (part // WIDE), unroll=True)
        def _(j):
            cols = pl.ds(pl.multiple_of(j * WIDE, WIDE), WIDE)
            on_diag = lax.broadcasted_iota(jnp.int32, (LANE, LANE), 0) == lax.broadcasted_iota(
                jnp.int32, (LANE, LANE), 1
            )
            units = []
            for k in range(per):
                here = pl.ds(pl.multiple_of(j * WIDE + k * LANE, LANE), LANE)
                gate_nat[j * per + k] = gate_ref[:, here].astype(F32)
                base_nat[j * per + k] = cand_ref[:, here].astype(F32)
                block = jnp.where(on_diag, blocks[j * per + k].astype(F32), 0.0)
                units.append(jnp.sum(block, axis=0, keepdims=True))
            unit = jnp.concatenate(units, axis=1)
            diag_ref[:, cols] = unit
            top = lax.broadcasted_iota(jnp.int32, (SUB, WIDE), 0) == 0
            rate = rates_ref[:, cols] * LOG2E
            mul, add = [], []
            for r in range(steps):
                here = pl.ds(r * SUB, SUB)
                gate = jnp.concatenate([gate_nat[j * per + k, turn[r], :] for k in range(per)], axis=1)
                base = jnp.concatenate([base_nat[j * per + k, turn[r], :] for k in range(per)], axis=1)
                keep = keep_of(gate, rate)
                keep_ref[here, cols] = keep
                base_ref[here, cols] = base
                left = 1.0 - keep
                cand = jnp.tanh(base + jnp.where(top, mixed[:, cols], 0.0) if r == 0 else base)
                slope = keep + left * (1.0 - cand * cand) * unit
                offset = left * cand
                if r == 0:
                    prev = jnp.where(top, init_ref[:, cols], 0.0)
                    offset = (keep * prev + offset) - slope * prev
                mul.append(slope)
                add.append(offset)
            cum_a, cum_b = chunk_scan(mul, add)
            for r in range(steps):
                here = pl.ds(r * SUB, SUB)
                cum_a_ref[here, cols] = cum_a[r]
                cum_b_ref[here, cols] = cum_b[r]
            write_rows(one, 0, j * per, cum_a[-1][SUB - 1 :, :])
            write_rows(one, tiles, j * per, cum_b[-1][SUB - 1 :, :])

    spread(one, pay_ref)


def step_kernel(
    last, me_ref, got_ref, init_ref, keep_ref, base_ref, cum_a_ref, cum_b_ref, diag_ref, w_ref, old_ref, tot_ref,
    *rest,
):
    if last:
        fresh_ref, out_a_ref, one, prev, low, entry, acc, mix = rest
    else:
        state_ref, out_a_ref, out_b_ref, sum_ref, pay_ref, prev, low, entry, one, acc, mix = rest
    rows, width = keep_ref.shape
    steps = rows // SUB
    tiles = width // LANE
    per = WIDE // LANE

    e = init_ref[...]
    order = order_of(got_ref.shape[0], int(last))
    for q in range(got_ref.shape[0] - 1):
        k = order.index(q)
        e = jnp.where(q < me_ref[0], got_ref[k, 0:tiles, :] * e + got_ref[k, tiles : 2 * tiles, :], e)
    entry[...] = e
    acc[...] = jnp.zeros_like(acc)

    def turned_state(j):
        cols = slice(j * WIDE, (j + 1) * WIDE)
        e = read_row(entry, j * per, per)
        state = [
            cum_b_ref[pl.ds(r * SUB, SUB), cols] + cum_a_ref[pl.ds(r * SUB, SUB), cols] * e for r in range(steps)
        ]
        place = lax.broadcasted_iota(jnp.int32, state[0].shape, 0)
        before = [jnp.where(place == 0, jnp.broadcast_to(e, state[0].shape), pltpu.roll(state[-1], 1, 0))] + state[:-1]
        moved = 0.0
        for r in range(steps):
            prev[pl.ds(r * SUB, SUB), cols] = before[r]
            change = state[r] if old_ref is None else state[r] - old_ref[pl.ds(r * SUB, SUB), cols]
            moved = moved + change * change
            if not last:
                state_ref[pl.ds(r * SUB, SUB), cols] = state[r]
        rounded = jnp.concatenate(before, axis=0).astype(BF16)
        low[:, cols] = rounded
        acc[...] += sum(moved[:, k * LANE : (k + 1) * LANE] for k in range(per))
        return jnp.dot(rounded, w_ref[cols, 0:WIDE], preferred_element_type=F32)

    mix[0] = sum(turned_state(j) for j in range(width // WIDE))
    if not last:
        sum_ref[...] = acc[...]
    else:
        one[pl.ds(4 * tiles, SUB), :] = jnp.zeros((SUB, LANE), F32)
        one[pl.ds(4 * tiles, 1), :] = jnp.sum(tot_ref[...], axis=0, keepdims=True)
        one[pl.ds(4 * tiles + 1, 1), :] = jnp.sum(acc[...], axis=0, keepdims=True)
        acc[...] = jnp.zeros_like(acc)

    def multiply(j, slot):
        cols = pl.ds(pl.multiple_of(j * WIDE, WIDE), WIDE)
        mix[slot] = jnp.dot(low[...], w_ref[:, cols], preferred_element_type=F32)

    def solve(j, slot):
        cols = pl.ds(pl.multiple_of(j * WIDE, WIDE), WIDE)
        unit = diag_ref[:, cols]
        mul, add = [], []
        for r in range(steps):
            here = pl.ds(r * SUB, SUB)
            keep = keep_ref[here, cols]
            before = prev[here, cols]
            cand = jnp.tanh(base_ref[here, cols] + mix[slot, here, :])
            left = 1.0 - keep
            mapped = keep * before + left * cand
            slope = keep + left * (1.0 - cand * cand) * unit
            mul.append(slope)
            add.append(mapped - slope * before)
        cum_a, cum_b = chunk_scan(mul, add)
        if last:
            e = read_row(entry, j * per, per)
            c0, c1, c2 = 0.0, 0.0, 0.0
            for r in range(steps):
                here = pl.ds(r * SUB, SUB)
                fresh = cum_b[r] + cum_a[r] * e
                if r + 1 < steps:
                    state = prev[pl.ds((r + 1) * SUB, SUB), cols]
                else:
                    state = cum_b_ref[here, cols] + cum_a_ref[here, cols] * e
                u = fresh - state
                for k in range(per):
                    part = slice(k * LANE, (k + 1) * LANE)
                    fresh_ref[j * per + k, pl.ds(r, SUB, stride=steps), :] = fresh[:, part]
                    out_a_ref[j * per + k, pl.ds(r, SUB, stride=steps), :] = cum_a[r][:, part]
                c0 = c0 + u * u
                c1 = c1 + u * cum_a[r]
                c2 = c2 + cum_a[r] * cum_a[r]
            acc[...] += sum(c0[:, k * LANE : (k + 1) * LANE] for k in range(per))
            write_rows(one, 0, j * per, cum_a[-1][SUB - 1 :, :])
            write_rows(one, tiles, j * per, u[SUB - 1 :, :])
            write_rows(one, 2 * tiles, j * per, 2.0 * jnp.sum(c1, axis=0, keepdims=True))
            write_rows(one, 3 * tiles, j * per, jnp.sum(c2, axis=0, keepdims=True))
        else:
            for r in range(steps):
                here = pl.ds(r * SUB, SUB)
                out_a_ref[here, cols] = cum_a[r]
                out_b_ref[here, cols] = cum_b[r]
            write_rows(one, 0, j * per, cum_a[-1][SUB - 1 :, :])
            write_rows(one, tiles, j * per, cum_b[-1][SUB - 1 :, :])

    blocks = width // WIDE

    @pl.loop(0, blocks // 2 - 1, unroll=True)
    def _(i):
        multiply(2 * i + 1, 1)
        solve(2 * i, 0)
        multiply(2 * i + 2, 0)
        solve(2 * i + 1, 1)

    multiply(blocks - 1, 1)
    solve(blocks - 2, 0)
    solve(blocks - 1, 1)
    if last:
        one[pl.ds(4 * tiles + 2, 1), :] = jnp.sum(acc[...], axis=0, keepdims=True)
    else:
        spread(one, pay_ref)


def first_step_kernel(me, got, init, keep, base, cum_a, cum_b, diag, w, *rest):
    step_kernel(False, me, got, init, keep, base, cum_a, cum_b, diag, w, None, None, *rest)


def pair_kernel(me_ref, one_ref, other_ref, pay_ref, both):
    tiles = (one_ref.shape[0] - SUB) // 4

    def join(first, second):
        a1, b1, l1, q1 = (first[k * tiles : (k + 1) * tiles, :] for k in range(4))
        a2, b2, l2, q2 = (second[k * tiles : (k + 1) * tiles, :] for k in range(4))
        both[0:tiles, :] = a1 * a2
        both[tiles : 2 * tiles, :] = a2 * b1 + b2
        both[2 * tiles : 3 * tiles, :] = l1 + a1 * (l2 + 2.0 * q2 * b1)
        both[3 * tiles : 4 * tiles, :] = q1 + a1 * a1 * q2
        both[4 * tiles :, :] = first[4 * tiles :, :] + second[4 * tiles :, :]
        extra = jnp.sum(b1 * (l2 + q2 * b1), axis=0, keepdims=True)
        both[4 * tiles + 2 : 4 * tiles + 3, :] = both[4 * tiles + 2 : 4 * tiles + 3, :] + extra

    @pl.when(lax.rem(me_ref[0], 2) == 0)
    def _():
        join(one_ref, other_ref)

    @pl.when(lax.rem(me_ref[0], 2) == 1)
    def _():
        join(other_ref, one_ref)

    spread(both, pay_ref)


def final_kernel(
    count, me_ref, got_ref, other_ref, fresh_ref, cum_a_ref, path_hbm, norm_hbm, moves, entry, path, norm_ref, sem
):
    tiles, rows, _ = fresh_ref.shape
    pairs = got_ref.shape[0]
    order = order_of(pairs, 2)
    moves[0] = jnp.zeros((tiles, LANE), F32)
    d = moves[0]
    for q in range(pairs - 1):
        k = order.index(q)
        d = got_ref[k, 0:tiles, :] * d + got_ref[k, tiles : 2 * tiles, :]
        moves[q + 1] = d
    entry[...] = moves[lax.div(me_ref[0], 2)]

    @pl.when(lax.rem(me_ref[0], 2) == 1)
    def _():
        entry[...] = other_ref[0:tiles, :] * entry[...] + other_ref[tiles : 2 * tiles, :]

    copies = []
    for p in range(CHUNKS):
        for j in range(p * tiles // CHUNKS, (p + 1) * tiles // CHUNKS):
            path[:, j * LANE : (j + 1) * LANE] = fresh_ref[j] + cum_a_ref[j] * entry[j : j + 1, :]
        here = pl.ds(p * (tiles // CHUNKS) * LANE, (tiles // CHUNKS) * LANE)
        copies.append(pltpu.make_async_copy(path.at[:, here], path_hbm.at[:, here], sem.at[p]))
        copies[-1].start()

    quad, sums = moves[0], moves[0, 0:SUB, :]
    for q in range(pairs):
        k = order.index(q)
        d = moves[q]
        quad = quad + d * (got_ref[k, 2 * tiles : 3 * tiles, :] + got_ref[k, 3 * tiles : 4 * tiles, :] * d)
        sums = sums + got_ref[k, 4 * tiles : 4 * tiles + SUB, :]
    extra = jnp.sum(quad, axis=0, keepdims=True)
    totals = [sums[0:1, :], sums[1:2, :], sums[2:3, :] + extra]
    for k, row in enumerate(totals):
        total = jnp.sum(row, axis=1, keepdims=True)
        norm_ref[k] = jnp.max(jnp.sqrt(total / count))
    copies.append(pltpu.make_async_copy(norm_ref, norm_hbm, sem.at[CHUNKS]))
    copies[-1].start()
    for copy in copies:
        copy.wait()


def order_of(count, stage):
    ends = [count - 1 - k // 2 if k % 2 == 0 else k // 2 for k in range(count)]
    return ORDERS.get((count, stage), ends)


def exchange(pay, stage, every=1):
    order = order_of(pay.shape[0], stage)
    return lax.all_to_all(pay, "tm", 0, 0, axis_index_groups=[[every * k + s for k in order] for s in range(every)])


def body(gate_in, cand_in, rates, init_state, recur_weight):
    rows, width = gate_in.shape
    peers = lax.axis_size("tm")
    tiles = width // LANE
    steps = rows // SUB
    assert rows % (2 * SUB) == 0 and width % (2 * WIDE) == 0 and peers % 2 == 0
    me = lax.axis_index("tm").astype(jnp.int32).reshape(1)
    init_row = init_state.reshape(1, width)
    init_tile = init_state.reshape(tiles, LANE)
    vmem = pl.BlockSpec(memory_space=pltpu.VMEM)
    smem = pl.BlockSpec(memory_space=pltpu.SMEM)
    hbm = pl.BlockSpec(memory_space=pltpu.HBM)
    grid_f32 = jax.ShapeDtypeStruct((rows, width), F32)
    pay2 = jax.ShapeDtypeStruct((peers, 2 * tiles, LANE), F32)
    last1 = jax.ShapeDtypeStruct((4 * tiles + SUB, LANE), F32)
    last8 = jax.ShapeDtypeStruct((peers // 2, 4 * tiles + SUB, LANE), F32)
    turned = jax.ShapeDtypeStruct((tiles, rows, LANE), F32)

    keep, base, cum_a, cum_b, diag, pay = pl.pallas_call(
        start_kernel,
        out_shape=(grid_f32, grid_f32, grid_f32, grid_f32, jax.ShapeDtypeStruct((1, width), F32), pay2),
        in_specs=[smem] + [hbm] * 5,
        out_specs=(vmem,) * 6,
        scratch_shapes=[
            pltpu.VMEM((rows, width), BF16),
            pltpu.VMEM((rows, width), BF16),
            pltpu.VMEM((1, width), F32),
            pltpu.VMEM((1, width), F32),
            pltpu.VMEM((width, width), BF16),
            pltpu.VMEM((tiles, LANE, LANE), BF16),
            pltpu.VMEM((tiles, rows, LANE), F32),
            pltpu.VMEM((tiles, rows, LANE), F32),
            pltpu.VMEM((1, width), F32),
            pltpu.VMEM((2 * tiles, LANE), F32),
            pltpu.SemaphoreType.DMA((2 * PARTS + 2,)),
            pltpu.SemaphoreType.DMA((PARTS,)),
            pltpu.SemaphoreType.DMA((tiles,)),
        ],
        compiler_params=pltpu.CompilerParams(vmem_limit_bytes=VMEM_LIMIT),
        name="start",
    )(me, *(pltpu.with_memory_space_constraint(x, pltpu.HBM) for x in (gate_in, cand_in, rates.reshape(1, width), init_row, recur_weight)))
    got = exchange(pay, 0)

    scratch = [
        pltpu.VMEM((rows, width), F32),
        pltpu.VMEM((rows, width), BF16),
        pltpu.VMEM((tiles, LANE), F32),
    ]
    tail = [pltpu.VMEM((SUB, LANE), F32), pltpu.VMEM((2, rows, WIDE), F32)]
    state, cum_a, cum_b, moved, pay = pl.pallas_call(
        first_step_kernel,
        out_shape=(grid_f32, grid_f32, grid_f32, jax.ShapeDtypeStruct((SUB, LANE), F32), pay2),
        in_specs=[smem] + [vmem] * 8,
        out_specs=(vmem,) * 5,
        scratch_shapes=scratch + [pltpu.VMEM((2 * tiles, LANE), F32)] + tail,
        compiler_params=pltpu.CompilerParams(vmem_limit_bytes=VMEM_LIMIT),
        name="middle",
    )(me, got, init_tile, keep, base, cum_a, cum_b, diag, recur_weight)
    got = exchange(pay, 1)

    fresh, cum_a, one = pl.pallas_call(
        functools.partial(step_kernel, True),
        out_shape=(turned, turned, last1),
        in_specs=[smem] + [vmem] * 10,
        out_specs=(vmem,) * 3,
        scratch_shapes=scratch + tail,
        compiler_params=pltpu.CompilerParams(vmem_limit_bytes=VMEM_LIMIT),
        name="last",
    )(me, got, init_tile, keep, base, cum_a, cum_b, diag, recur_weight, state, moved)

    other = lax.ppermute(one, "tm", [(k, k ^ 1) for k in range(peers)])
    pay = pl.pallas_call(
        pair_kernel,
        out_shape=last8,
        in_specs=[smem] + [vmem] * 2,
        out_specs=vmem,
        scratch_shapes=[pltpu.VMEM(last1.shape, F32)],
        compiler_params=pltpu.CompilerParams(vmem_limit_bytes=VMEM_LIMIT),
        name="pair",
    )(me, one, other)
    got = exchange(pay, 2, every=2)

    path, norms = pl.pallas_call(
        functools.partial(final_kernel, peers * rows * width),
        out_shape=(grid_f32, jax.ShapeDtypeStruct((3,), F32)),
        in_specs=[smem] + [vmem] * 4,
        out_specs=(hbm, hbm),
        scratch_shapes=[
            pltpu.VMEM((peers // 2, tiles, LANE), F32),
            pltpu.VMEM((tiles, LANE), F32),
            pltpu.VMEM((rows, width), F32),
            pltpu.SMEM((3,), F32),
            pltpu.SemaphoreType.DMA((CHUNKS + 1,)),
        ],
        compiler_params=pltpu.CompilerParams(vmem_limit_bytes=VMEM_LIMIT),
        name="final",
    )(me, got, other, fresh, cum_a)
    return path, norms


def solution(mesh):
    placed = (P("tm", "batch"), P("tm", "batch"), P("batch"), P("batch"), P())
    return jax.shard_map(
        body, mesh=mesh, in_specs=placed, out_specs=(P("tm", "batch"), P("batch")), check_vma=False
    )
```
